32 devices in a mesh: dp: 2 (over z, core), sp: 16 (over x, y).
Axes of the slice: x: 4, y: 4, z: 1, core: 2. Of those that a mesh axis runs over, the one named last changes fastest.
The devices are a block of a 4x4x8 slice.
Arguments:
- x: bfloat16 [16384, 2304], P(('dp', 'sp')), parts along dimension 0
- gain: bfloat16 [2304], replicated
- wq: bfloat16 [2304, 2048], P('sp')
- wk: bfloat16 [2304, 1024], P('sp')
- wv: bfloat16 [2304, 1024], P('sp')
- wo: bfloat16 [2048, 2304], P('sp')
Outputs:
- output: bfloat16 [16384, 2304], P(('dp', 'sp')), parts along dimension 0
There are 2 independent parts. The reference program is written for one: setup_inputs(seed, part) draws one part's arguments, and reference() takes and returns one part's arrays. A program takes and returns all parts, laid end to end along the dimension named above; an argument that names none is the same for every part.
All inputs are finite; a program needn't handle non-finite values.
Results may differ from the reference program's by a relative error of at most 0.012.
Values are sent between devices in bfloat16 or wider.
A program may use at most 768 MiB of HBM per device.

```python
import jax
import jax.numpy as jnp
from jax import lax

ROWS = 8192
D = 2304
HEADS = 8
KV_HEADS = 4
HEAD = 256
THETA = 10000


def setup_inputs(seed: int = 0, part: int = 0) -> dict:
    kx, kn, kq, kk, kv, ko = jax.random.split(jax.random.key(seed), 6)

    def weights(key, rows, columns):
        return jax.random.normal(key, (rows, columns), jnp.float32) * rows**-0.5

    drawn = {
        "x": jax.random.normal(jax.random.fold_in(kx, part), (ROWS, D), jnp.float32),
        "gain": 1 + 0.1 * jax.random.normal(kn, (D,), jnp.float32),
        "wq": 2 * weights(kq, D, HEADS * HEAD),
        "wk": 2 * weights(kk, D, KV_HEADS * HEAD),
        "wv": 4 * weights(kv, D, KV_HEADS * HEAD),
        "wo": weights(ko, HEADS * HEAD, D),
    }
    return {k: v.astype(jnp.bfloat16) for k, v in drawn.items()}


def normed(x, gain):
    wide = x.astype(jnp.float32)
    scale = lax.rsqrt(jnp.mean(wide * wide, -1, keepdims=True) + 1e-6)
    return (wide * scale * gain.astype(jnp.float32)).astype(jnp.bfloat16)


def turned(t, place, theta):
    half = t.shape[-1] // 2
    angle = place.astype(jnp.float32)[:, None] * theta ** (-jnp.arange(half, dtype=jnp.float32) / half)
    cos, sin = jnp.cos(angle)[:, None], jnp.sin(angle)[:, None]
    a, b = t[..., :half].astype(jnp.float32), t[..., half:].astype(jnp.float32)
    return jnp.concatenate([a * cos - b * sin, b * cos + a * sin], -1).astype(jnp.bfloat16)


def matmul(a, w):
    return jnp.dot(a, w, preferred_element_type=jnp.float32).astype(jnp.bfloat16)


def einsum(form, a, b):
    return jnp.einsum(form, a.astype(jnp.float32), b.astype(jnp.float32))


def attention(q, k, v):
    scores = einsum("tgsd,ugd->gstu", q, k) * q.shape[-1] ** -0.5
    token = jnp.arange(q.shape[0])
    scores = jnp.where(token[:, None] >= token, scores, -jnp.inf)
    weights = jax.nn.softmax(scores, -1).astype(jnp.bfloat16)
    return einsum("gstu,ugd->tgsd", weights, v).astype(jnp.bfloat16)


def reference(x, gain, wq, wk, wv, wo):
    a, place = normed(x, gain), jnp.arange(ROWS)
    q = turned(matmul(a, wq).reshape(ROWS, HEADS, HEAD), place, THETA).reshape(ROWS, KV_HEADS, -1, HEAD)
    k = turned(matmul(a, wk).reshape(ROWS, KV_HEADS, HEAD), place, THETA)
    v = matmul(a, wv).reshape(ROWS, KV_HEADS, HEAD)
    seen = attention(q, k, v).reshape(ROWS, HEADS * HEAD)
    return (x.astype(jnp.float32) + jnp.dot(seen, wo, preferred_element_type=jnp.float32)).astype(jnp.bfloat16)
```

```python
import functools
import math

import jax
import jax.numpy as jnp
import numpy as np
from jax import lax
from jax.experimental import pallas as pl
from jax.experimental.pallas import tpu as pltpu
from jax.sharding import PartitionSpec as P

HEAD = 256
THETA = 10000
NEG = -1e30
HIDDEN = 2 * NEG
LOG2E = 1.4426950408889634
MESH = pl.DeviceIdType.MESH

PIECES = ((0, 0), (0, 1), (-1, 0), (1, 1), (-1, 1), (1, 0), (2, 0), (2, 1))


def pick(t, values):
    out = jnp.int32(values[-1])
    for i in range(len(values) - 2, -1, -1):
        out = jnp.where(t == i, jnp.int32(values[i]), out)
    return out


def dot(a, b, ca, cb):
    return lax.dot_general(a, b, (((ca,), (cb,)), ((), ())), preferred_element_type=jnp.float32)


def kernel(n, g, x_ref, gain_ref, wq_ref, wk_ref, wv_ref, wo_ref, cosr_ref, sinr_ref, cosc_ref, sinc_ref, y_ref,
           xbuf, xn, wbuf, wobuf, qbuf, kbuf, vbuf, mix, top, sout, seen,
           x_s, x_r, w1_s, w1_r, w_l, w2_s, w2_r, w3_s, w3_r, o1_s, o1_r, o_l, o2_s, o2_r, o3_s, o3_r, kv_s, kv_r, a_s, a_r):
    own, d = x_ref.shape
    half = own // 2
    rows = wq_ref.shape[0]
    orow = wo_ref.shape[0] // 2
    width = g * HEAD
    sp, dp = lax.axis_index("sp"), lax.axis_index("dp")
    X, Y = lax.div(sp, n), lax.rem(sp, n)
    c = lax.rem(dp, 2)
    partner = {"dp": dp + 1 - 2 * c}

    def at(v, by):
        return lax.rem(v + n + by, n)

    def on_x(by):
        return {"sp": at(X, by) * n + Y}

    def on_y(by):
        return {"sp": X * n + at(Y, by)}

    def send(src, dst, ss, rs, dev):
        pltpu.make_async_remote_copy(src_ref=src, dst_ref=dst, send_sem=ss, recv_sem=rs, device_id=dev, device_id_type=MESH).start()

    def got(dst, rs):
        pltpu.make_async_remote_copy(src_ref=dst, dst_ref=dst, send_sem=rs, recv_sem=rs, device_id=partner, device_id_type=MESH).wait_recv()

    def sent(src, ss):
        pltpu.make_async_remote_copy(src_ref=src, dst_ref=src, send_sem=ss, recv_sem=ss, device_id=partner, device_id_type=MESH).wait_send()

    def local(src, dst, sem):
        pltpu.make_async_copy(src, dst, sem).start()

    barrier = pltpu.get_barrier_semaphore()
    peers = [on_x(by) for by in range(1, n)] + [on_y(1), on_y(-1), partner]
    for peer in peers:
        pl.semaphore_signal(barrier, inc=1, device_id=peer, device_id_type=MESH)
    pl.semaphore_wait(barrier, len(peers))

    mine = pl.ds(pl.multiple_of(c * width, width), width)

    def w_dst(xi, p):
        return wbuf.at[xi, Y, :, pl.ds(pl.multiple_of(c * width + p * HEAD, HEAD), HEAD)]

    def w_begin(srcs):
        for by in range(1, n):
            for p in range(2):
                send(srcs(at(X, by), p), w_dst(X, p), w1_s.at[by - 1, p], w1_r.at[by - 1, p], on_x(by))
        for p in range(2):
            local(srcs(X, p), w_dst(X, p), w_l.at[p])

    @pl.when(c == 0)
    def _():
        w_begin(lambda h, p: wq_ref.at[:, pl.ds(pl.multiple_of(h * width + p * HEAD, HEAD), HEAD)])

    @pl.when(c == 1)
    def _():
        w_begin(lambda h, p: (wk_ref, wv_ref)[p].at[:, pl.ds(pl.multiple_of(h * HEAD, HEAD), HEAD)])

    def x_piece(by, hf):
        return xbuf.at[at(X, by), pl.ds(hf * half, half), :]

    for hf in range(2):
        local(x_ref.at[pl.ds(hf * half, half), :], x_piece(0, hf), x_r.at[hf])
    for i, (by, hf, k) in enumerate(((1, 0, 2), (-1, 1, 3), (1, 1, 4), (-1, 0, 5))):
        send(x_ref.at[pl.ds(hf * half, half), :], x_piece(0, hf), x_s.at[i], x_r.at[k], on_x(by))

    wide = d // 2

    def o_cols(o):
        return pl.ds(o * wide, wide)

    def o_first(o, by):
        return on_y(by) if o == 0 else on_x(by)

    def o_second(o, by):
        return on_x(by) if o == 0 else on_y(by)

    def o_block(o, by, lo=0, size=orow, core=None):
        core = c if core is None else core
        xi, yi = (X, at(Y, by)) if o == 0 else (at(X, by), Y)
        return wobuf.at[xi, yi, core, pl.ds(lo, size), o_cols(o)]

    def o_line(o, by, lo=0, size=n, core=None):
        core = c if core is None else core
        if o == 0:
            return wobuf.at[at(X, by), pl.ds(lo, size), core, :, o_cols(o)]
        return wobuf.at[pl.ds(lo, size), at(Y, by), core, :, o_cols(o)]

    def o1_begin(o):
        src = wo_ref.at[pl.ds(pl.multiple_of(c * orow, orow), orow), o_cols(o)]
        send(src, o_block(o, 0), o1_s.at[o, 0], o1_r.at[o, 0], o_first(o, 1))
        send(src, o_block(o, 0), o1_s.at[o, 1], o1_r.at[o, 1], o_first(o, -1))
        local(src, o_block(o, 0), o_l.at[o])

    hr = orow // 2

    def o1_forward(o):
        got(o_block(o, -1), o1_r.at[o, 0])
        send(o_block(o, -1, 0, hr), o_block(o, -1, 0, hr), o1_s.at[o, 2], o1_r.at[o, 2], o_first(o, 1))
        got(o_block(o, 1), o1_r.at[o, 1])
        send(o_block(o, 1, hr, hr), o_block(o, 1, hr, hr), o1_s.at[o, 3], o1_r.at[o, 3], o_first(o, -1))

    def o3(o, k, by):
        send(o_line(o, by), o_line(o, by), o3_s.at[o, k], o3_r.at[o, k], partner)

    def o2_begin(o):
        got(o_block(o, 2, 0, hr), o1_r.at[o, 2])
        got(o_block(o, 2, hr, hr), o1_r.at[o, 3])
        pltpu.make_async_copy(o_block(o, 0), o_block(o, 0), o_l.at[o]).wait()
        send(o_line(o, 0), o_line(o, 0), o2_s.at[o, 0], o2_r.at[o, 0], o_second(o, 1))
        send(o_line(o, 0), o_line(o, 0), o2_s.at[o, 1], o2_r.at[o, 1], o_second(o, -1))
        o3(o, 0, 0)

    hn = n // 2

    def o2_forward(o):
        got(o_line(o, -1), o2_r.at[o, 0])
        send(o_line(o, -1, 0, hn), o_line(o, -1, 0, hn), o2_s.at[o, 2], o2_r.at[o, 2], o_second(o, 1))
        got(o_line(o, 1), o2_r.at[o, 1])
        send(o_line(o, 1, hn, hn), o_line(o, 1, hn, hn), o2_s.at[o, 3], o2_r.at[o, 3], o_second(o, -1))
        o3(o, 1, -1)
        o3(o, 2, 1)

    def o2_finish(o):
        got(o_line(o, 2, 0, hn), o2_r.at[o, 2])
        got(o_line(o, 2, hn, hn), o2_r.at[o, 3])
        o3(o, 3, 2)

    def o_wait(o):
        for k, by in enumerate((0, -1, 1, 2)):
            got(o_line(o, by, core=1 - c), o3_r.at[o, k])

    o1_begin(0)

    top[...] = jnp.full(top.shape, NEG, jnp.float32)

    @pl.loop(0, n)
    def _(m):
        mix[m] = jnp.zeros(mix.shape[1:], jnp.float32)

    for by in range(1, n):
        for p in range(2):
            got(w_dst(at(X, -by), p), w1_r.at[by - 1, p])
    for p in range(2):
        pltpu.make_async_copy(w_dst(X, p), w_dst(X, p), w_l.at[p]).wait()

    def w_line(by, lo=0, size=n, cols=mine):
        return wbuf.at[pl.ds(lo, size), at(Y, by), :, cols]

    def w3(k, by):
        send(w_line(by), w_line(by), w3_s.at[k], w3_r.at[k], partner)

    send(w_line(0), w_line(0), w2_s.at[0], w2_r.at[0], on_y(1))
    send(w_line(0), w_line(0), w2_s.at[1], w2_r.at[1], on_y(-1))
    w3(0, 0)
    o1_forward(0)
    got(w_line(-1), w2_r.at[0])
    send(w_line(-1, 0, hn), w_line(-1, 0, hn), w2_s.at[2], w2_r.at[2], on_y(1))
    w3(1, -1)
    got(w_line(1), w2_r.at[1])
    send(w_line(1, hn, hn), w_line(1, hn, hn), w2_s.at[3], w2_r.at[3], on_y(-1))
    w3(2, 1)
    got(w_line(2, 0, hn), w2_r.at[2])
    got(w_line(2, hn, hn), w2_r.at[3])
    w3(3, 2)
    theirs = pl.ds(pl.multiple_of((1 - c) * width, width), width)
    for k, by in enumerate((0, -1, 1, 2)):
        got(w_line(by, cols=theirs), w3_r.at[k])

    def piece_of(p):
        return at(X, pick(p, [by for by, _ in PIECES])), pick(p, [hf for _, hf in PIECES]) * half

    def k_part(p, by):
        m, lo = piece_of(p)
        return kbuf.at[at(Y, by), m, pl.ds(pl.multiple_of(lo, half), half), :]

    def v_part(p, by):
        m, lo = piece_of(p)
        return vbuf.at[at(Y, by), m, :, pl.ds(pl.multiple_of(lo, half), half)]

    def kv_send(p):
        for kind, part, by in ((0, k_part, 1), (1, k_part, -1), (2, v_part, 1), (3, v_part, -1)):
            send(part(p, 0), part(p, 0), kv_s.at[p, kind], kv_r.at[p, kind], on_y(by))

    def kv_forward(p):
        got(k_part(p, -1), kv_r.at[p, 0])
        send(k_part(p, -1), k_part(p, -1), kv_s.at[p, 4], kv_r.at[p, 4], on_y(1))
        got(v_part(p, 1), kv_r.at[p, 3])
        send(v_part(p, 1), v_part(p, 1), kv_s.at[p, 5], kv_r.at[p, 5], on_y(-1))

    def kv_near(p):
        got(k_part(p, 1), kv_r.at[p, 1])
        got(v_part(p, -1), kv_r.at[p, 2])

    def kv_far(p):
        got(k_part(p, 2), kv_r.at[p, 4])
        got(v_part(p, 2), kv_r.at[p, 5])

    step = 32

    def project(p):
        m, lo = piece_of(p)
        lo = pl.multiple_of(lo, half)
        place = m * n + Y

        @pl.loop(0, half // step)
        def _(i):
            here = pl.ds(pl.multiple_of(i * step, step), step)
            t = xbuf[m, pl.ds(pl.multiple_of(lo + i * step, step), step), :].astype(jnp.float32)
            scale = lax.rsqrt(jnp.mean(t * t, -1, keepdims=True) + 1e-6)
            xn[here, :] = (t * scale * gain_ref[...].astype(jnp.float32)).astype(jnp.bfloat16)

        def columns(i):
            w = wbuf[:, :, :, i * HEAD : (i + 1) * HEAD].reshape(n * n * rows, HEAD)
            return dot(xn[...], w, 1, 0).astype(jnp.bfloat16)

        cc, sc = cosc_ref[pl.ds(place, 1), :], sinc_ref[pl.ds(place, 1), :]

        def turned(t):
            cr, sr = cosr_ref[pl.ds(lo, half), :], sinr_ref[pl.ds(lo, half), :]
            cos, sin = cc * cr - sc * sr, sc * cr + cc * sr
            a, b = t[:, : HEAD // 2].astype(jnp.float32), t[:, HEAD // 2 :].astype(jnp.float32)
            return jnp.concatenate([a * cos - b * sin, b * cos + a * sin], -1).astype(jnp.bfloat16)

        kbuf[Y, m, pl.ds(lo, half), :] = turned(columns(g))
        vbuf[Y, m, :, pl.ds(lo, half)] = columns(g + 1).T
        for h in range(g):
            qbuf[m, pl.ds(pl.multiple_of(h * own + lo, half), half), :] = turned(columns(h))

    e = HEAD**-0.5 * LOG2E

    def tile(mq, j, mk, masked):
        keys = kbuf[j, mk]
        scores = [dot(keys, qbuf[mq, h * own : (h + 1) * own, :], 1, 1) for h in range(g)]
        weights, keeps = [], []
        for h, s in enumerate(scores):
            at_h = slice(h * own, (h + 1) * own)
            if masked:
                ok = lax.broadcasted_iota(jnp.int32, s.shape, 0) <= lax.broadcasted_iota(jnp.int32, s.shape, 1)
                s = jnp.where(ok, s, HIDDEN)
            old = top[mq, :, at_h]
            new = jnp.maximum(old, s.max(axis=0, keepdims=True))
            top[mq, :, at_h] = new
            weights.append(jnp.exp2((s - new) * e).astype(jnp.bfloat16))
            keeps.append(jnp.exp2((old - new) * e))
        values = jnp.concatenate([vbuf[j, mk], jnp.ones((8, own), jnp.bfloat16)], axis=0)
        for h in range(g):
            at_h = slice(h * own, (h + 1) * own)
            mix[mq, :, at_h] = mix[mq, :, at_h] * keeps[h] + dot(values, weights[h], 1, 0)

    def attend(ra, rb, by):
        ma, mb = at(X, ra), at(X, rb)
        mq, mk, j = jnp.maximum(ma, mb), jnp.minimum(ma, mb), at(Y, by)
        q_place, k_place = mq * n + Y, mk * n + j

        @pl.when(k_place == q_place)
        def _():
            tile(mq, j, mk, True)

        @pl.when(k_place < q_place)
        def _():
            tile(mq, j, mk, False)

    def tasks(table, before):
        def body(t, _):
            for i, todo in before.items():

                @pl.when(t == i)
                def _(todo=todo):
                    todo()

            attend(*(pick(t, [row[k] for row in table]) for k in range(3)))

        lax.fori_loop(0, len(table), body, None)

    def cross(pairs, *places):
        return [(a, b, by) for by in places for a, b in pairs]

    def each(f, *ps):
        return lambda: [f(p) for p in ps]

    def finish(mq):
        out = mix[mq, :HEAD, :] * (1 / mix[mq, HEAD : HEAD + 1, :])
        for h in range(g):
            sout[mq, :, h * HEAD : (h + 1) * HEAD] = out[:, h * own : (h + 1) * own].T.astype(jnp.bfloat16)

        @pl.when(mq == X)
        def _():
            seen[X] = sout[mq]

        @pl.when(mq != X)
        def _():
            send(sout.at[mq], seen.at[X], a_s.at[mq], a_r.at[X], {"sp": mq * n + Y})

    second = [(0, -1), (0, 1), (-1, 1), (-1, -1), (1, 1)]
    third = [(2, 0), (2, -1), (2, 1), (2, 2)]

    @pl.loop(0, len(PIECES))
    def _(p):
        got(xbuf.at[0, pl.ds(0, half), :], x_r.at[p])

        @pl.when(p == 2)
        def _():
            send(x_piece(-1, 0), x_piece(-1, 0), x_s.at[4], x_r.at[6], on_x(1))

        @pl.when(p == 3)
        def _():
            send(x_piece(1, 1), x_piece(1, 1), x_s.at[5], x_r.at[7], on_x(-1))

        project(p)
        kv_send(p)

        @pl.when((p >= 2) & (p < 6))
        def _():
            kv_forward(p - 2)

        @pl.when(p == 3)
        def _():
            o1_begin(1)
            o2_begin(0)
            tasks(cross([(0, 0)], 0, 1, -1, 2), {1: each(kv_near, 0, 1), 3: each(kv_far, 0, 1)})

        @pl.when(p == 5)
        def _():
            tasks(cross(second, 0, 1, -1), {5: lambda: (each(kv_forward, 4, 5)(), each(kv_near, 2, 3, 4, 5)())})

    last = at(X, 2)

    def send_on():
        o1_forward(1)

    def early():
        @pl.loop(0, n)
        def _(mq):
            @pl.when(mq < last)
            def _():
                finish(mq)

        o2_begin(1)

    def passed():
        each(kv_forward, 6, 7)()
        o2_forward(0)
        each(kv_near, 6, 7)()

    def final():
        each(kv_far, 6, 7)()

    tasks(
        cross(second, 2) + cross(third, 0, 1, -1, 2),
        {0: lambda: (o1_forward(1), each(kv_far, 2, 3, 4, 5)()), 5: early, 9: passed, 17: final},
    )

    @pl.loop(1, n + 1)
    def _(by):
        mq = at(X, by)

        @pl.when(mq >= last)
        def _():
            finish(mq)

    o2_forward(1)
    o2_finish(0)
    o2_finish(1)
    o_wait(0)
    o_wait(1)

    for by in range(1, n):
        got(seen.at[at(X, by)], a_r.at[at(X, by)])

    tn = 256

    @pl.loop(0, d // tn)
    def _(i):
        here = pl.ds(pl.multiple_of(i * tn, tn), tn)
        total = xbuf[X, :, here].astype(jnp.float32)
        acc = None
        for h in range(n):
            part = dot(seen[h], wobuf[h, :, :, :, here].reshape(width, tn), 1, 0)
            acc = part if acc is None else acc + part
        y_ref[:, here] = (total + acc).astype(y_ref.dtype)

    for i, hf in enumerate((0, 1, 1, 0, 0, 1)):
        sent(x_piece(0, hf), x_s.at[i])
    for by in range(1, n):
        for p in range(2):
            sent(w_dst(X, p), w1_s.at[by - 1, p])
    for i in range(4):
        sent(w_line(0) if i < 2 else w_line(0, 0, hn), w2_s.at[i])
        sent(w_line(0), w3_s.at[i])
        for o in range(2):
            sent(o_block(o, 0) if i < 2 else o_block(o, 0, 0, hr), o1_s.at[o, i])
            sent(o_line(o, 0) if i < 2 else o_line(o, 0, 0, hn), o2_s.at[o, i])
            sent(o_line(o, 0), o3_s.at[o, i])

    @pl.loop(0, len(PIECES))
    def _(p):
        for kind, part in enumerate((k_part, k_part, v_part, v_part, k_part, v_part)):
            sent(part(p, 0), kv_s.at[p, kind])

    for by in range(1, n):
        sent(sout.at[at(X, by)], a_s.at[at(X, by)])


def tables(own, chunks):
    half = HEAD // 2
    rate = np.float64(THETA) ** (-np.arange(half, dtype=np.float64) / half)
    row = np.arange(own, dtype=np.float64)[:, None] * rate
    chunk = (np.arange(chunks, dtype=np.float64) * own)[:, None] * rate
    return [f(t).astype(np.float32) for t in (row, chunk) for f in (np.cos, np.sin)]


def solution(mesh):
    n = math.isqrt(mesh.shape["sp"])

    def step(x, gain, wq, wk, wv, wo):
        own, d = x.shape
        g = wq.shape[1] // wk.shape[1]
        rows, orow = wq.shape[0], wo.shape[0] // 2
        cosr, sinr, cosc, sinc = tables(own, n * n)
        hbm, vmem = pl.BlockSpec(memory_space=pl.ANY), pl.BlockSpec(memory_space=pltpu.VMEM)
        bf, dma = jnp.bfloat16, pltpu.SemaphoreType.DMA
        return pl.pallas_call(
            functools.partial(kernel, n, g),
            out_shape=jax.ShapeDtypeStruct(x.shape, bf),
            in_specs=[hbm, vmem, hbm, hbm, hbm, hbm, vmem, vmem, vmem, vmem],
            out_specs=vmem,
            scratch_shapes=[
                pltpu.VMEM((n, own, d), bf),
                pltpu.VMEM((own // 2, d), bf),
                pltpu.VMEM((n, n, rows, 2 * g * HEAD), bf),
                pltpu.VMEM((n, n, 2, orow, d), bf),
                pltpu.VMEM((n, g * own, HEAD), bf),
                pltpu.VMEM((n, n, own, HEAD), bf),
                pltpu.VMEM((n, n, HEAD, own), bf),
                pltpu.VMEM((n, HEAD + 8, g * own), jnp.float32),
                pltpu.VMEM((n, 1, g * own), jnp.float32),
                pltpu.VMEM((n, own, g * HEAD), bf),
                pltpu.VMEM((n, own, g * HEAD), bf),
                dma((6,)), dma((8,)),
                dma((3, 2)), dma((3, 2)), dma((2,)),
                dma((4,)), dma((4,)), dma((4,)), dma((4,)),
                dma((2, 4)), dma((2, 4)), dma((2,)),
                dma((2, 4)), dma((2, 4)), dma((2, 4)), dma((2, 4)),
                dma((8, 6)), dma((8, 6)),
                dma((n,)), dma((n,)),
            ],
            compiler_params=pltpu.CompilerParams(collective_id=0, has_side_effects=True, vmem_limit_bytes=66_000_000),
        )(x, gain.reshape(1, d), wq, wk, wv, wo, cosr, sinr, cosc, sinc)

    tokens, whole = P(("dp", "sp"), None), P("sp", None)
    return jax.shard_map(
        step,
        mesh=mesh,
        in_specs=(tokens, P(None), whole, whole, whole, whole),
        out_specs=tokens,
        check_vma=False,
    )
```

```python
import functools
import math

import jax
import jax.numpy as jnp
import numpy as np
from jax import lax
from jax.experimental import pallas as pl
from jax.experimental.pallas import tpu as pltpu
from jax.sharding import PartitionSpec as P

HEAD = 256
THETA = 10000
NEG = -1e30
HIDDEN = 2 * NEG
LOG2E = 1.4426950408889634
MESH = pl.DeviceIdType.MESH

PIECES = ((0, 0, 2), (0, 2, 2), (-1, 0, 2), (1, 2, 2), (-1, 2, 2), (1, 0, 2), (2, 0, 1), (2, 2, 1), (2, 1, 1), (2, 3, 1))


def pick(t, values):
    out = jnp.int32(values[-1])
    for i in range(len(values) - 2, -1, -1):
        out = jnp.where(t == i, jnp.int32(values[i]), out)
    return out


def dot(a, b, ca, cb):
    return lax.dot_general(a, b, (((ca,), (cb,)), ((), ())), preferred_element_type=jnp.float32)


def kernel(n, g, x_ref, gain_ref, wq_ref, wk_ref, wv_ref, wo_ref, cosr_ref, sinr_ref, cosc_ref, sinc_ref, y_ref,
           xbuf, xn, wbuf, wobuf, qbuf, kbuf, vbuf, mix, top, sout, seen, relay, acc,
           x_s, x_r, w1_s, w1_r, w_l, w2_s, w2_r, w3_s, w3_r, o1_s, o1_r, o_l, o2_s, o2_r, o3_s, o3_r, kv_s, kv_r, a_s, a_r, r_s, r_r):
    own, d = x_ref.shape
    half, quarter = own // 2, own // 4
    rows = wq_ref.shape[0]
    orow = wo_ref.shape[0] // 2
    width = g * HEAD
    sp, dp = lax.axis_index("sp"), lax.axis_index("dp")
    X, Y = lax.div(sp, n), lax.rem(sp, n)
    c = lax.rem(dp, 2)
    partner = {"dp": dp + 1 - 2 * c}

    def at(v, by):
        return lax.rem(v + n + by, n)

    def on_x(by):
        return {"sp": at(X, by) * n + Y}

    def on_y(by):
        return {"sp": X * n + at(Y, by)}

    def send(src, dst, ss, rs, dev):
        pltpu.make_async_remote_copy(src_ref=src, dst_ref=dst, send_sem=ss, recv_sem=rs, device_id=dev, device_id_type=MESH).start()

    def got(dst, rs):
        pltpu.make_async_remote_copy(src_ref=dst, dst_ref=dst, send_sem=rs, recv_sem=rs, device_id=partner, device_id_type=MESH).wait_recv()

    def sent(src, ss):
        pltpu.make_async_remote_copy(src_ref=src, dst_ref=src, send_sem=ss, recv_sem=ss, device_id=partner, device_id_type=MESH).wait_send()

    def local(src, dst, sem):
        pltpu.make_async_copy(src, dst, sem).start()

    barrier = pltpu.get_barrier_semaphore()
    peers = [on_x(by) for by in range(1, n)] + [on_y(by) for by in range(1, n)] + [partner]
    for peer in peers:
        pl.semaphore_signal(barrier, inc=1, device_id=peer, device_id_type=MESH)
    pl.semaphore_wait(barrier, len(peers))

    def block(f, core):
        return pl.ds(pl.multiple_of((2 * f + core) * HEAD, HEAD), HEAD)

    def w_dst(f, xi):
        return wbuf.at[xi, Y, :, block(f, c)]

    def w_begin(f, src):
        for by in (1, n - 1, 2):
            send(src(at(X, by)), w_dst(f, X), w1_s.at[f, by - 1], w1_r.at[f, by - 1], on_x(by))
        local(src(X), w_dst(f, X), w_l.at[f])

    def head_of(ref):
        return lambda h: ref.at[:, pl.ds(pl.multiple_of(h * HEAD, HEAD), HEAD)]

    @pl.when(c == 0)
    def _():
        w_begin(0, head_of(wk_ref))

    @pl.when(c == 1)
    def _():
        w_begin(0, head_of(wv_ref))

    w_begin(1, lambda h: wq_ref.at[:, pl.ds(pl.multiple_of(h * width + c * HEAD, HEAD), HEAD)])

    def x_rows(by, lo, size):
        return xbuf.at[at(X, by), pl.ds(lo * quarter, size * quarter), :]

    for p in range(2):
        _, lo, size = PIECES[p]
        local(x_ref.at[pl.ds(lo * quarter, size * quarter), :], x_rows(0, lo, size), x_r.at[p])
    for i, p in enumerate((2, 3, 4, 5)):
        by, lo, size = PIECES[p]
        send(x_ref.at[pl.ds(lo * quarter, size * quarter), :], x_rows(0, lo, size), x_s.at[i], x_r.at[p], on_x(-by))

    def x_forward(p):
        by = PIECES[p][0]
        for k in (0, 2):
            _, lo, size = PIECES[p + 4 + k]
            send(x_rows(by, lo, size), x_rows(by, lo, size), x_s.at[p + 2 + k], x_r.at[p + 4 + k], on_x(-by))

    cut = d // (3 * 128) * 128

    def o_cols(o):
        return pl.ds(0, cut) if o == 0 else pl.ds(cut, d - cut)

    def o_first(o, by):
        return on_y(by) if o == 0 else on_x(by)

    def o_second(o, by):
        return on_x(by) if o == 0 else on_y(by)

    def o_block(o, by):
        xi, yi = (X, at(Y, by)) if o == 0 else (at(X, by), Y)
        return wobuf.at[xi, yi, c, :, o_cols(o)]

    def o_line(o, by, lo=0, size=n, core=None):
        core = c if core is None else core
        if o == 0:
            return wobuf.at[at(X, by), pl.ds(lo, size), core, :, o_cols(o)]
        return wobuf.at[pl.ds(lo, size), at(Y, by), core, :, o_cols(o)]

    def o1_begin(o):
        src = wo_ref.at[pl.ds(pl.multiple_of(c * orow, orow), orow), o_cols(o)]
        for by in range(1, n):
            send(src, o_block(o, 0), o1_s.at[o, by - 1], o1_r.at[o, by - 1], o_first(o, by))
        local(src, o_block(o, 0), o_l.at[o])

    def o3(o, k, by):
        send(o_line(o, by), o_line(o, by), o3_s.at[o, k], o3_r.at[o, k], partner)

    def o2_begin(o):
        for by in range(1, n):
            got(o_block(o, -by), o1_r.at[o, by - 1])
        pltpu.make_async_copy(o_block(o, 0), o_block(o, 0), o_l.at[o]).wait()
        send(o_line(o, 0), o_line(o, 0), o2_s.at[o, 0], o2_r.at[o, 0], o_second(o, 1))
        send(o_line(o, 0), o_line(o, 0), o2_s.at[o, 1], o2_r.at[o, 1], o_second(o, -1))
        o3(o, 0, 0)

    hn = n // 2

    def o2_forward(o):
        got(o_line(o, -1), o2_r.at[o, 0])
        send(o_line(o, -1, 0, hn), o_line(o, -1, 0, hn), o2_s.at[o, 2], o2_r.at[o, 2], o_second(o, 1))
        got(o_line(o, 1), o2_r.at[o, 1])
        send(o_line(o, 1, hn, hn), o_line(o, 1, hn, hn), o2_s.at[o, 3], o2_r.at[o, 3], o_second(o, -1))
        o3(o, 1, -1)
        o3(o, 2, 1)

    def o2_finish(o):
        got(o_line(o, 2, 0, hn), o2_r.at[o, 2])
        got(o_line(o, 2, hn, hn), o2_r.at[o, 3])
        o3(o, 3, 2)

    def o_wait(o):
        for k, by in enumerate((0, -1, 1, 2)):
            got(o_line(o, by, core=1 - c), o3_r.at[o, k])

    o1_begin(0)

    step = 32

    def piece_of(p):
        lo = pl.multiple_of(pick(p, [lo for _, lo, _ in PIECES]) * quarter, quarter)
        return at(X, pick(p, [by for by, _, _ in PIECES])), lo

    def norm(p, size):
        m, lo = piece_of(p)
        slot = lax.rem(p, 2)

        @pl.loop(0, size * quarter // step)
        def _(i):
            here = pl.ds(pl.multiple_of(i * step, step), step)
            t = xbuf[m, pl.ds(pl.multiple_of(lo + i * step, step), step), :].astype(jnp.float32)
            scale = lax.rsqrt(jnp.mean(t * t, -1, keepdims=True) + 1e-6)
            xn[slot, here, :] = (t * scale * gain_ref[...].astype(jnp.float32)).astype(jnp.bfloat16)

    def columns(p, size, i):
        w = wbuf[:, :, :, i * HEAD : (i + 1) * HEAD].reshape(n * n * rows, HEAD)
        return dot(xn[lax.rem(p, 2), : size * quarter, :], w, 1, 0).astype(jnp.bfloat16)

    def turned(t, m, lo):
        place = m * n + Y
        cc, sc = cosc_ref[pl.ds(place, 1), :], sinc_ref[pl.ds(place, 1), :]
        cr, sr = cosr_ref[pl.ds(lo, t.shape[0]), :], sinr_ref[pl.ds(lo, t.shape[0]), :]
        cos, sin = cc * cr - sc * sr, sc * cr + cc * sr
        a, b = t[:, : HEAD // 2].astype(jnp.float32), t[:, HEAD // 2 :].astype(jnp.float32)
        return jnp.concatenate([a * cos - b * sin, b * cos + a * sin], -1).astype(jnp.bfloat16)

    def keys_values(p, size):
        m, lo = piece_of(p)
        kbuf[Y, m, pl.ds(lo, size * quarter), :] = turned(columns(p, size, 0), m, lo)
        vbuf[Y, m, :, pl.ds(lo, size * quarter)] = columns(p, size, 1).T

    def queries(p, size):
        m, lo = piece_of(p)
        for h in range(g):
            qbuf[m, pl.ds(pl.multiple_of(h * own + lo, quarter), size * quarter), :] = turned(columns(p, size, 2 + h), m, lo)

    def k_part(p, size, by):
        m, lo = piece_of(p)
        return kbuf.at[at(Y, by), m, pl.ds(lo, size * quarter), :]

    def v_part(p, size, by):
        m, lo = piece_of(p)
        return vbuf.at[at(Y, by), m, :, pl.ds(lo, size * quarter)]

    def kv_send(p, size):
        for kind, part, by in ((0, k_part, 1), (1, k_part, -1), (2, v_part, 1), (3, v_part, -1)):
            send(part(p, size, 0), part(p, size, 0), kv_s.at[p, kind], kv_r.at[p, kind], on_y(by))

    def kv_forward(*ps):
        for p in ps:
            k, v = k_part(p, PIECES[p][2], -1), v_part(p, PIECES[p][2], 1)
            got(k, kv_r.at[p, 0])
            send(k, k, kv_s.at[p, 4], kv_r.at[p, 4], on_y(1))
            got(v, kv_r.at[p, 3])
            send(v, v, kv_s.at[p, 5], kv_r.at[p, 5], on_y(-1))

    def kv_near(*ps):
        for p in ps:
            got(k_part(p, PIECES[p][2], 1), kv_r.at[p, 1])
            got(v_part(p, PIECES[p][2], -1), kv_r.at[p, 2])

    def kv_far(*ps):
        for p in ps:
            got(k_part(p, PIECES[p][2], 2), kv_r.at[p, 4])
            got(v_part(p, PIECES[p][2], 2), kv_r.at[p, 5])

    e = HEAD**-0.5 * LOG2E

    def tile(mq, j, mk, masked):
        keys = kbuf[j, mk]
        scores = [dot(keys, qbuf[mq, h * own : (h + 1) * own, :], 1, 1) for h in range(g)]
        weights, keeps = [], []
        for h, s in enumerate(scores):
            at_h = slice(h * own, (h + 1) * own)
            if masked:
                ok = lax.broadcasted_iota(jnp.int32, s.shape, 0) <= lax.broadcasted_iota(jnp.int32, s.shape, 1)
                s = jnp.where(ok, s, HIDDEN)
            old = top[mq, :, at_h]
            new = jnp.maximum(old, s.max(axis=0, keepdims=True))
            top[mq, :, at_h] = new
            weights.append(jnp.exp2((s - new) * e).astype(jnp.bfloat16))
            keeps.append(jnp.exp2((old - new) * e))
        values = jnp.concatenate([vbuf[j, mk], jnp.ones((8, own), jnp.bfloat16)], axis=0)
        for h in range(g):
            at_h = slice(h * own, (h + 1) * own)
            mix[mq, :, at_h] = mix[mq, :, at_h] * keeps[h] + dot(values, weights[h], 1, 0)

    def attend(ra, rb, by):
        ma, mb = at(X, ra), at(X, rb)
        mq, mk, j = jnp.maximum(ma, mb), jnp.minimum(ma, mb), at(Y, by)
        q_place, k_place = mq * n + Y, mk * n + j

        @pl.when(k_place == q_place)
        def _():
            tile(mq, j, mk, True)

        @pl.when(k_place < q_place)
        def _():
            tile(mq, j, mk, False)

    def tasks(table, before):
        def body(t, _):
            for i, todo in before.items():

                @pl.when(t == i)
                def _(todo=todo):
                    todo()

            attend(*(pick(t, [row[k] for row in table]) for k in range(3)))

        lax.fori_loop(0, len(table), body, None)

    def cross(pairs, *places):
        return [(a, b, by) for by in places for a, b in pairs]

    last = at(X, 2)

    def finish(mq):
        out = mix[mq, :HEAD, :] * (1 / mix[mq, HEAD : HEAD + 1, :])

        def put(ref):
            for h in range(g):
                ref[mq if ref is sout else X, :, h * HEAD : (h + 1) * HEAD] = out[:, h * own : (h + 1) * own].T.astype(jnp.bfloat16)

        put(sout)

        @pl.when(mq == X)
        def _():
            seen[X] = sout[mq]

        @pl.when(mq == last)
        def _():
            send(sout.at[mq, pl.ds(half, half), :], relay, r_s.at[0], r_r, on_x(-1))
            send(sout.at[mq, pl.ds(0, half), :], seen.at[X, pl.ds(0, half), :], a_s.at[mq], a_r.at[X, 0], on_x(2))

        @pl.when((mq != X) & (mq != last))
        def _():
            send(sout.at[mq], seen.at[X], a_s.at[mq], a_r.at[X, 0], {"sp": mq * n + Y})

    def pass_on():
        got(relay, r_r)
        send(relay, seen.at[at(X, 1), pl.ds(half, half), :], r_s.at[1], a_r.at[at(X, 1), 1], on_x(-1))

    top[...] = jnp.full(top.shape, NEG, jnp.float32)

    @pl.loop(0, n)
    def _(m):
        mix[m] = jnp.zeros(mix.shape[1:], jnp.float32)

    def arrive(p, size):
        got(xbuf.at[0, pl.ds(0, size * quarter), :], x_r.at[p])

    def pair(a, size, f):
        lax.fori_loop(a, a + 2, lambda p, _: f(p, size), None)

    def early_half(p, size):
        norm(p, size)
        keys_values(p, size)
        kv_send(p, size)

    arrive(0, 2)
    arrive(1, 2)
    pair(0, 2, norm)

    def w_line(f, by, lo=0, size=n, core=None):
        return wbuf.at[pl.ds(lo, size), at(Y, by), :, block(f, c if core is None else core)]

    def w3(f, k, by):
        send(w_line(f, by), w_line(f, by), w3_s.at[f, k], w3_r.at[f, k], partner)

    def w2_begin(f):
        for by in range(1, n):
            got(w_dst(f, at(X, -by)), w1_r.at[f, by - 1])
        pltpu.make_async_copy(w_dst(f, X), w_dst(f, X), w_l.at[f]).wait()
        send(w_line(f, 0), w_line(f, 0), w2_s.at[f, 0], w2_r.at[f, 0], on_y(1))
        send(w_line(f, 0), w_line(f, 0), w2_s.at[f, 1], w2_r.at[f, 1], on_y(-1))
        w3(f, 0, 0)

    def w2_forward(f):
        got(w_line(f, -1), w2_r.at[f, 0])
        send(w_line(f, -1, 0, hn), w_line(f, -1, 0, hn), w2_s.at[f, 2], w2_r.at[f, 2], on_y(1))
        got(w_line(f, 1), w2_r.at[f, 1])
        send(w_line(f, 1, hn, hn), w_line(f, 1, hn, hn), w2_s.at[f, 3], w2_r.at[f, 3], on_y(-1))
        w3(f, 1, -1)
        w3(f, 2, 1)

    def w2_finish(f):
        got(w_line(f, 2, 0, hn), w2_r.at[f, 2])
        got(w_line(f, 2, hn, hn), w2_r.at[f, 3])
        w3(f, 3, 2)

    def w3_wait(f):
        for k, by in enumerate((0, -1, 1, 2)):
            got(w_line(f, by, core=1 - c), w3_r.at[f, k])

    w2_begin(0)
    w2_forward(0)
    w2_begin(1)
    w2_finish(0)
    w3_wait(0)

    @pl.loop(0, 2)
    def _(p):
        keys_values(p, 2)
        kv_send(p, 2)

    w2_forward(1)
    w2_finish(1)
    w3_wait(1)
    pair(0, 2, queries)

    for p in (2, 3):
        arrive(p, 2)
        x_forward(p)
    pair(2, 2, early_half)
    kv_forward(0, 1)
    pair(2, 2, queries)
    o1_begin(1)
    o2_begin(0)
    tasks(cross([(0, 0)], 0, 1, -1), {1: lambda: kv_near(0, 1)})
    kv_forward(2, 3)

    arrive(4, 2)
    arrive(5, 2)
    pair(4, 2, early_half)
    pair(4, 2, queries)
    second = [(0, -1), (0, 1), (-1, 1), (-1, -1), (1, 1)]
    third = [(2, 0), (2, -1), (2, 1), (2, 2)]
    tasks(cross([(0, 0)], 2) + cross(second, 0), {0: lambda: kv_far(0, 1)})

    arrive(6, 1)
    arrive(7, 1)
    pair(6, 1, early_half)
    pair(6, 1, queries)
    tasks(cross(second, 1, -1), {0: lambda: (kv_forward(4, 5), kv_near(2, 3, 4, 5))})
    kv_forward(6, 7)

    arrive(8, 1)
    arrive(9, 1)
    pair(8, 1, early_half)
    pair(8, 1, queries)

    def early():
        @pl.loop(0, n)
        def _(mq):
            @pl.when(mq < last)
            def _():
                finish(mq)

    tasks(
        cross(second, 2) + cross(third, 0, 1, -1, 2),
        {
            0: lambda: kv_far(2, 3, 4, 5),
            5: early,
            9: lambda: (kv_forward(8, 9), o2_begin(1), o2_forward(0), kv_near(6, 7, 8, 9)),
            17: lambda: kv_far(6, 7, 8, 9),
        },
    )

    @pl.loop(2, n + 2)
    def _(by):
        mq = at(X, pick(by, (0, 0, 2, 1, 3, 0)))

        @pl.when(mq >= last)
        def _():
            finish(mq)

    pass_on()
    o2_finish(0)
    o2_forward(1)
    o2_finish(1)
    o_wait(0)
    o_wait(1)

    tn = 256

    def out_head(h, first=False, final=False):
        @pl.loop(0, d // tn)
        def _(i):
            here = pl.ds(pl.multiple_of(i * tn, tn), tn)
            part = dot(seen[h], wobuf[h, :, :, :, here].reshape(width, tn), 1, 0)
            total = part + (xbuf[X, :, here].astype(jnp.float32) if first else acc[:, here])
            if final:
                y_ref[:, here] = total.astype(y_ref.dtype)
            else:
                acc[:, here] = total

    out_head(X, first=True)

    @pl.loop(0, 2)
    def _(i):
        h = at(X, pick(i, (1, -1)))
        got(seen.at[h], a_r.at[h, 0])
        out_head(h)

    got(seen.at[last, pl.ds(0, half), :], a_r.at[last, 0])
    got(seen.at[last, pl.ds(half, half), :], a_r.at[last, 1])
    out_head(last, final=True)

    for i in range(8):
        sent(x_rows(0, 0, PIECES[i + 2][2]), x_s.at[i])
    for f in range(2):
        for by in range(1, n):
            sent(w_dst(f, X), w1_s.at[f, by - 1])
        for i in range(4):
            sent(w_line(f, 0) if i < 2 else w_line(f, 0, 0, hn), w2_s.at[f, i])
            sent(w_line(f, 0), w3_s.at[f, i])
    for o in range(2):
        for by in range(1, n):
            sent(o_block(o, 0), o1_s.at[o, by - 1])
        for i in range(4):
            sent(o_line(o, 0) if i < 2 else o_line(o, 0, 0, hn), o2_s.at[o, i])
            sent(o_line(o, 0), o3_s.at[o, i])
    for p in range(len(PIECES)):
        for kind, part in enumerate((k_part, k_part, v_part, v_part, k_part, v_part)):
            sent(part(p, PIECES[p][2], 0), kv_s.at[p, kind])
    for by in (1, -1):
        sent(sout.at[at(X, by)], a_s.at[at(X, by)])
    sent(relay, a_s.at[last])
    sent(relay, r_s.at[0])
    sent(relay, r_s.at[1])


def tables(own, chunks):
    half = HEAD // 2
    rate = np.float64(THETA) ** (-np.arange(half, dtype=np.float64) / half)
    row = np.arange(own, dtype=np.float64)[:, None] * rate
    chunk = (np.arange(chunks, dtype=np.float64) * own)[:, None] * rate
    return [f(t).astype(np.float32) for t in (row, chunk) for f in (np.cos, np.sin)]


def solution(mesh):
    n = math.isqrt(mesh.shape["sp"])

    def step(x, gain, wq, wk, wv, wo):
        own, d = x.shape
        g = wq.shape[1] // wk.shape[1]
        rows, orow = wq.shape[0], wo.shape[0] // 2
        cosr, sinr, cosc, sinc = tables(own, n * n)
        hbm, vmem = pl.BlockSpec(memory_space=pl.ANY), pl.BlockSpec(memory_space=pltpu.VMEM)
        bf, dma = jnp.bfloat16, pltpu.SemaphoreType.DMA
        return pl.pallas_call(
            functools.partial(kernel, n, g),
            out_shape=jax.ShapeDtypeStruct(x.shape, bf),
            in_specs=[hbm, vmem, hbm, hbm, hbm, hbm, vmem, vmem, vmem, vmem],
            out_specs=vmem,
            scratch_shapes=[
                pltpu.VMEM((n, own, d), bf),
                pltpu.VMEM((2, own // 2, d), bf),
                pltpu.VMEM((n, n, rows, 2 * g * HEAD), bf),
                pltpu.VMEM((n, n, 2, orow, d), bf),
                pltpu.VMEM((n, g * own, HEAD), bf),
                pltpu.VMEM((n, n, own, HEAD), bf),
                pltpu.VMEM((n, n, HEAD, own), bf),
                pltpu.VMEM((n, HEAD + 8, g * own), jnp.float32),
                pltpu.VMEM((n, 1, g * own), jnp.float32),
                pltpu.VMEM((n, own, g * HEAD), bf),
                pltpu.VMEM((n, own, g * HEAD), bf),
                pltpu.VMEM((own // 2, g * HEAD), bf),
                pltpu.VMEM((own, d), jnp.float32),
                dma((8,)), dma((len(PIECES),)),
                dma((2, n - 1)), dma((2, n - 1)), dma((2,)),
                dma((2, 4)), dma((2, 4)), dma((2, 4)), dma((2, 4)),
                dma((2, n - 1)), dma((2, n - 1)), dma((2,)),
                dma((2, 4)), dma((2, 4)), dma((2, 4)), dma((2, 4)),
                dma((len(PIECES), 6)), dma((len(PIECES), 6)),
                dma((n,)), dma((n, 2)), dma((2,)), dma(()),
            ],
            compiler_params=pltpu.CompilerParams(collective_id=0, has_side_effects=True, vmem_limit_bytes=66_000_000),
        )(x, gain.reshape(1, d), wq, wk, wv, wo, cosr, sinr, cosc, sinc)

    tokens, whole = P(("dp", "sp"), None), P("sp", None)
    return jax.shard_map(
        step,
        mesh=mesh,
        in_specs=(tokens, P(None), whole, whole, whole, whole),
        out_specs=tokens,
        check_vma=False,
    )
```

```python
import functools
import math

import jax
import jax.numpy as jnp
import numpy as np
from jax import lax
from jax.experimental import pallas as pl
from jax.experimental.pallas import tpu as pltpu
from jax.sharding import PartitionSpec as P

HEAD = 256
THETA = 10000
NEG = -1e30
HIDDEN = 2 * NEG
LOG2E = 1.4426950408889634
MESH = pl.DeviceIdType.MESH

PIECES = ((0, 0, 2), (0, 2, 2), (-1, 0, 2), (1, 2, 2), (-1, 2, 2), (1, 0, 2), (2, 0, 1), (2, 2, 1), (2, 1, 1), (2, 3, 1))


def pick(t, values):
    out = jnp.int32(values[-1])
    for i in range(len(values) - 2, -1, -1):
        out = jnp.where(t == i, jnp.int32(values[i]), out)
    return out


def dot(a, b, ca, cb):
    return lax.dot_general(a, b, (((ca,), (cb,)), ((), ())), preferred_element_type=jnp.float32)


def kernel(n, g, x_ref, gain_ref, wq_ref, wk_ref, wv_ref, wo_ref, cosr_ref, sinr_ref, cosc_ref, sinc_ref, y_ref,
           xbuf, xn, wbuf, wobuf, qbuf, kbuf, vbuf, mix, top, sout, seen, relay, acc, yout,
           x_s, x_r, w1_s, w1_r, w_l, w2_s, w2_r, w3_s, w3_r, o1_s, o1_r, o_l, o2_s, o2_r, o3_s, o3_r, kv_s, kv_r, a_s, a_r, r_s, r_r, y_s):
    own, d = x_ref.shape
    half, quarter = own // 2, own // 4
    rows = wq_ref.shape[0]
    orow = wo_ref.shape[0] // 2
    width = g * HEAD
    sp, dp = lax.axis_index("sp"), lax.axis_index("dp")
    X, Y = lax.div(sp, n), lax.rem(sp, n)
    c = lax.rem(dp, 2)
    partner = {"dp": dp + 1 - 2 * c}

    def at(v, by):
        return lax.rem(v + n + by, n)

    def on_x(by):
        return {"sp": at(X, by) * n + Y}

    def on_y(by):
        return {"sp": X * n + at(Y, by)}

    def send(src, dst, ss, rs, dev):
        pltpu.make_async_remote_copy(src_ref=src, dst_ref=dst, send_sem=ss, recv_sem=rs, device_id=dev, device_id_type=MESH).start()

    def got(dst, rs):
        pltpu.make_async_remote_copy(src_ref=dst, dst_ref=dst, send_sem=rs, recv_sem=rs, device_id=partner, device_id_type=MESH).wait_recv()

    def sent(src, ss):
        pltpu.make_async_remote_copy(src_ref=src, dst_ref=src, send_sem=ss, recv_sem=ss, device_id=partner, device_id_type=MESH).wait_send()

    def local(src, dst, sem):
        pltpu.make_async_copy(src, dst, sem).start()

    barrier = pltpu.get_barrier_semaphore()
    peers = [on_x(by) for by in range(1, n)] + [on_y(by) for by in range(1, n)] + [partner]
    for peer in peers:
        pl.semaphore_signal(barrier, inc=1, device_id=peer, device_id_type=MESH)
    pl.semaphore_wait(barrier, len(peers))

    def block(f, core):
        return pl.ds(pl.multiple_of((2 * f + core) * HEAD, HEAD), HEAD)

    def w_dst(f, xi):
        return wbuf.at[xi, Y, :, block(f, c)]

    def w_begin(f, src):
        for by in (1, n - 1, 2):
            send(src(at(X, by)), w_dst(f, X), w1_s.at[f, by - 1], w1_r.at[f, by - 1], on_x(by))
        local(src(X), w_dst(f, X), w_l.at[f])

    def head_of(ref):
        return lambda h: ref.at[:, pl.ds(pl.multiple_of(h * HEAD, HEAD), HEAD)]

    @pl.when(c == 0)
    def _():
        w_begin(0, head_of(wk_ref))

    @pl.when(c == 1)
    def _():
        w_begin(0, head_of(wv_ref))

    w_begin(1, lambda h: wq_ref.at[:, pl.ds(pl.multiple_of(h * width + c * HEAD, HEAD), HEAD)])

    def x_rows(by, lo, size):
        return xbuf.at[at(X, by), pl.ds(lo * quarter, size * quarter), :]

    for p in range(2):
        _, lo, size = PIECES[p]
        local(x_ref.at[pl.ds(lo * quarter, size * quarter), :], x_rows(0, lo, size), x_r.at[p])
    for i, p in enumerate((2, 3, 4, 5)):
        by, lo, size = PIECES[p]
        send(x_ref.at[pl.ds(lo * quarter, size * quarter), :], x_rows(0, lo, size), x_s.at[i], x_r.at[p], on_x(-by))

    def x_forward(p):
        by = PIECES[p][0]
        for k in (0, 2):
            _, lo, size = PIECES[p + 4 + k]
            send(x_rows(by, lo, size), x_rows(by, lo, size), x_s.at[p + 2 + k], x_r.at[p + 4 + k], on_x(-by))

    cut = d // (2 * 128) * 128

    def o_cols(o):
        return pl.ds(0, cut) if o == 0 else pl.ds(cut, d - cut)

    def o_first(o, by):
        return on_y(by) if o == 0 else on_x(by)

    def o_second(o, by):
        return on_x(by) if o == 0 else on_y(by)

    def o_block(o, by):
        xi, yi = (X, at(Y, by)) if o == 0 else (at(X, by), Y)
        return wobuf.at[xi, yi, c, :, o_cols(o)]

    def o_line(o, by, lo=0, size=n, core=None):
        core = c if core is None else core
        if o == 0:
            return wobuf.at[at(X, by), pl.ds(lo, size), core, :, o_cols(o)]
        return wobuf.at[pl.ds(lo, size), at(Y, by), core, :, o_cols(o)]

    def o1_begin(o):
        src = wo_ref.at[pl.ds(pl.multiple_of(c * orow, orow), orow), o_cols(o)]
        for by in range(1, n):
            send(src, o_block(o, 0), o1_s.at[o, by - 1], o1_r.at[o, by - 1], o_first(o, by))
        local(src, o_block(o, 0), o_l.at[o])

    def o3(o, k, by):
        send(o_line(o, by), o_line(o, by), o3_s.at[o, k], o3_r.at[o, k], partner)

    def o2_begin(o):
        for by in range(1, n):
            got(o_block(o, -by), o1_r.at[o, by - 1])
        pltpu.make_async_copy(o_block(o, 0), o_block(o, 0), o_l.at[o]).wait()
        send(o_line(o, 0), o_line(o, 0), o2_s.at[o, 0], o2_r.at[o, 0], o_second(o, 1))
        send(o_line(o, 0), o_line(o, 0), o2_s.at[o, 1], o2_r.at[o, 1], o_second(o, -1))
        o3(o, 0, 0)

    hn = n // 2

    def o2_forward(o):
        got(o_line(o, -1), o2_r.at[o, 0])
        send(o_line(o, -1, 0, hn), o_line(o, -1, 0, hn), o2_s.at[o, 2], o2_r.at[o, 2], o_second(o, 1))
        got(o_line(o, 1), o2_r.at[o, 1])
        send(o_line(o, 1, hn, hn), o_line(o, 1, hn, hn), o2_s.at[o, 3], o2_r.at[o, 3], o_second(o, -1))
        o3(o, 1, -1)
        o3(o, 2, 1)

    def o2_finish(o):
        got(o_line(o, 2, 0, hn), o2_r.at[o, 2])
        got(o_line(o, 2, hn, hn), o2_r.at[o, 3])
        o3(o, 3, 2)

    def o_wait(o):
        for k, by in enumerate((0, -1, 1, 2)):
            got(o_line(o, by, core=1 - c), o3_r.at[o, k])

    o1_begin(0)

    step = 32

    def piece_of(p):
        lo = pl.multiple_of(pick(p, [lo for _, lo, _ in PIECES]) * quarter, quarter)
        return at(X, pick(p, [by for by, _, _ in PIECES])), lo

    def norm(p, size):
        m, lo = piece_of(p)
        slot = lax.rem(p, 2)

        @pl.loop(0, size * quarter // step)
        def _(i):
            here = pl.ds(pl.multiple_of(i * step, step), step)
            t = xbuf[m, pl.ds(pl.multiple_of(lo + i * step, step), step), :].astype(jnp.float32)
            scale = lax.rsqrt(jnp.mean(t * t, -1, keepdims=True) + 1e-6)
            xn[slot, here, :] = (t * scale * gain_ref[...].astype(jnp.float32)[None, :]).astype(jnp.bfloat16)

    def columns(p, size, i):
        w = wbuf[:, :, :, i * HEAD : (i + 1) * HEAD].reshape(n * n * rows, HEAD)
        return dot(xn[lax.rem(p, 2), : size * quarter, :], w, 1, 0).astype(jnp.bfloat16)

    def turned(t, m, lo):
        place = m * n + Y
        cc, sc = cosc_ref[pl.ds(place, 1), :], sinc_ref[pl.ds(place, 1), :]
        cr, sr = cosr_ref[pl.ds(lo, t.shape[0]), :], sinr_ref[pl.ds(lo, t.shape[0]), :]
        cos, sin = cc * cr - sc * sr, sc * cr + cc * sr
        a, b = t[:, : HEAD // 2].astype(jnp.float32), t[:, HEAD // 2 :].astype(jnp.float32)
        return jnp.concatenate([a * cos - b * sin, b * cos + a * sin], -1).astype(jnp.bfloat16)

    def keys_values(p, size):
        m, lo = piece_of(p)
        kbuf[Y, m, pl.ds(lo, size * quarter), :] = turned(columns(p, size, 0), m, lo)
        vbuf[Y, m, :, pl.ds(lo, size * quarter)] = columns(p, size, 1).T

    def queries(p, size):
        m, lo = piece_of(p)
        for h in range(g):
            qbuf[m, pl.ds(pl.multiple_of(h * own + lo, quarter), size * quarter), :] = turned(columns(p, size, 2 + h), m, lo)

    def k_part(p, size, by):
        m, lo = piece_of(p)
        return kbuf.at[at(Y, by), m, pl.ds(lo, size * quarter), :]

    def v_part(p, size, by):
        m, lo = piece_of(p)
        return vbuf.at[at(Y, by), m, :, pl.ds(lo, size * quarter)]

    def kv_send(p, size):
        for kind, part, by in ((0, k_part, 1), (1, k_part, -1), (2, v_part, 1), (3, v_part, -1)):
            send(part(p, size, 0), part(p, size, 0), kv_s.at[p, kind], kv_r.at[p, kind], on_y(by))

    def kv_forward(*ps):
        for p in ps:
            k, v = k_part(p, PIECES[p][2], -1), v_part(p, PIECES[p][2], 1)
            got(k, kv_r.at[p, 0])
            send(k, k, kv_s.at[p, 4], kv_r.at[p, 4], on_y(1))
            got(v, kv_r.at[p, 3])
            send(v, v, kv_s.at[p, 5], kv_r.at[p, 5], on_y(-1))

    def kv_near(*ps):
        for p in ps:
            got(k_part(p, PIECES[p][2], 1), kv_r.at[p, 1])
            got(v_part(p, PIECES[p][2], -1), kv_r.at[p, 2])

    def kv_far(*ps):
        for p in ps:
            got(k_part(p, PIECES[p][2], 2), kv_r.at[p, 4])
            got(v_part(p, PIECES[p][2], 2), kv_r.at[p, 5])

    e = HEAD**-0.5 * LOG2E

    def tile(mq, j, mk, masked):
        keys = kbuf[j, mk]
        scores = [dot(keys, qbuf[mq, h * own : (h + 1) * own, :], 1, 1) for h in range(g)]
        weights, keeps = [], []
        for h, s in enumerate(scores):
            at_h = slice(h * own, (h + 1) * own)
            if masked:
                ok = lax.broadcasted_iota(jnp.int32, s.shape, 0) <= lax.broadcasted_iota(jnp.int32, s.shape, 1)
                s = jnp.where(ok, s, HIDDEN)
            old = top[mq, :, at_h]
            new = jnp.maximum(old, s.max(axis=0, keepdims=True))
            top[mq, :, at_h] = new
            weights.append(jnp.exp2((s - new) * e).astype(jnp.bfloat16))
            keeps.append(jnp.exp2((old - new) * e))
        values = jnp.concatenate([vbuf[j, mk], jnp.ones((8, own), jnp.bfloat16)], axis=0)
        for h in range(g):
            at_h = slice(h * own, (h + 1) * own)
            mix[mq, :, at_h] = mix[mq, :, at_h] * keeps[h] + dot(values, weights[h], 1, 0)

    def attend(ra, rb, by):
        ma, mb = at(X, ra), at(X, rb)
        mq, mk, j = jnp.maximum(ma, mb), jnp.minimum(ma, mb), at(Y, by)
        q_place, k_place = mq * n + Y, mk * n + j

        @pl.when(k_place == q_place)
        def _():
            tile(mq, j, mk, True)

        @pl.when(k_place < q_place)
        def _():
            tile(mq, j, mk, False)

    def tasks(table, before):
        def body(t, _):
            for i, todo in before.items():

                @pl.when(t == i)
                def _(todo=todo):
                    todo()

            attend(*(pick(t, [row[k] for row in table]) for k in range(3)))

        lax.fori_loop(0, len(table), body, None)

    def cross(pairs, *places):
        return [(a, b, by) for by in places for a, b in pairs]

    last = at(X, 2)
    slots = (0, 1, 3, 2)

    def seat(rel, lo=0, size=own):
        return seen.at[pl.ds(lo, size), pl.ds(pl.multiple_of(pick(rel, slots) * width, width), width)]

    def finish(mq):
        out = mix[mq, :HEAD, :] * (1 / mix[mq, HEAD : HEAD + 1, :])
        to = at(mq, -X)
        back = at(X, -mq)
        for h in range(g):
            sout[mq, :, h * HEAD : (h + 1) * HEAD] = out[:, h * own : (h + 1) * own].T.astype(jnp.bfloat16)

        @pl.when(to == 0)
        def _():
            seen[:, :width] = sout[mq]

        @pl.when(to == 2)
        def _():
            send(sout.at[mq, pl.ds(half, half), :], relay, r_s.at[0], r_r, on_x(-1))
            send(sout.at[mq, pl.ds(0, half), :], seat(2, 0, half), a_s.at[mq], a_r.at[2], on_x(2))

        @pl.when((to == 1) | (to == 3))
        def _():
            send(sout.at[mq], seat(back), a_s.at[mq], a_r.at[back], {"sp": mq * n + Y})

    def pass_on():
        got(relay, r_r)
        send(relay, seat(2, half, half), r_s.at[1], a_r.at[0], on_x(-1))

    top[...] = jnp.full(top.shape, NEG, jnp.float32)

    @pl.loop(0, n)
    def _(m):
        mix[m] = jnp.zeros(mix.shape[1:], jnp.float32)

    def arrive(p, size):
        got(xbuf.at[0, pl.ds(0, size * quarter), :], x_r.at[p])

    def pair(a, size, f):
        lax.fori_loop(a, a + 2, lambda p, _: f(p, size), None)

    def early_half(p, size):
        norm(p, size)
        keys_values(p, size)
        kv_send(p, size)

    arrive(0, 2)
    arrive(1, 2)
    pair(0, 2, norm)

    def w_line(f, by, lo=0, size=n, core=None):
        return wbuf.at[pl.ds(lo, size), at(Y, by), :, block(f, c if core is None else core)]

    def w3(f, k, by):
        send(w_line(f, by), w_line(f, by), w3_s.at[f, k], w3_r.at[f, k], partner)

    def w2_begin(f):
        for by in range(1, n):
            got(w_dst(f, at(X, -by)), w1_r.at[f, by - 1])
        pltpu.make_async_copy(w_dst(f, X), w_dst(f, X), w_l.at[f]).wait()
        send(w_line(f, 0), w_line(f, 0), w2_s.at[f, 0], w2_r.at[f, 0], on_y(1))
        send(w_line(f, 0), w_line(f, 0), w2_s.at[f, 1], w2_r.at[f, 1], on_y(-1))
        w3(f, 0, 0)

    def w2_forward(f):
        got(w_line(f, -1), w2_r.at[f, 0])
        send(w_line(f, -1, 0, hn), w_line(f, -1, 0, hn), w2_s.at[f, 2], w2_r.at[f, 2], on_y(1))
        got(w_line(f, 1), w2_r.at[f, 1])
        send(w_line(f, 1, hn, hn), w_line(f, 1, hn, hn), w2_s.at[f, 3], w2_r.at[f, 3], on_y(-1))
        w3(f, 1, -1)
        w3(f, 2, 1)

    def w2_finish(f):
        got(w_line(f, 2, 0, hn), w2_r.at[f, 2])
        got(w_line(f, 2, hn, hn), w2_r.at[f, 3])
        w3(f, 3, 2)

    def w3_wait(f):
        for k, by in enumerate((0, -1, 1, 2)):
            got(w_line(f, by, core=1 - c), w3_r.at[f, k])

    w2_begin(0)
    w2_forward(0)
    w2_begin(1)
    w2_finish(0)
    w3_wait(0)
    pair(0, 2, keys_values)
    w2_forward(1)
    pair(0, 2, kv_send)
    w2_finish(1)
    w3_wait(1)
    pair(0, 2, queries)

    for p in (2, 3):
        arrive(p, 2)
        x_forward(p)
    pair(2, 2, early_half)
    kv_forward(0, 1)
    pair(2, 2, queries)
    o1_begin(1)
    o2_begin(0)
    tasks(cross([(0, 0)], 0, 1, -1), {1: lambda: kv_near(0, 1)})
    kv_forward(2, 3)

    arrive(4, 2)
    arrive(5, 2)
    pair(4, 2, early_half)
    pair(4, 2, queries)
    second = [(0, -1), (0, 1), (-1, 1), (-1, -1), (1, 1)]
    third = [(2, 0), (2, -1), (2, 1), (2, 2)]
    tasks(cross([(0, 0)], 2) + cross(second, 0), {0: lambda: kv_far(0, 1)})

    arrive(6, 1)
    arrive(7, 1)
    pair(6, 1, early_half)
    pair(6, 1, queries)
    tasks(cross(second, 1, -1), {0: lambda: (kv_forward(4, 5), kv_near(2, 3, 4, 5))})
    kv_forward(6, 7)

    arrive(8, 1)
    arrive(9, 1)
    pair(8, 1, early_half)
    o2_begin(1)
    pair(8, 1, queries)

    def early():
        @pl.loop(0, n)
        def _(mq):
            @pl.when(mq < last)
            def _():
                finish(mq)

    tasks(
        cross(second, 2) + cross(third, 0, 1, -1, 2),
        {
            0: lambda: kv_far(2, 3, 4, 5),
            5: early,
            9: lambda: (kv_forward(8, 9), o2_forward(0), kv_near(6, 7, 8, 9)),
            17: lambda: kv_far(6, 7, 8, 9),
        },
    )

    @pl.loop(2, n + 2)
    def _(by):
        mq = at(X, pick(by, (0, 0, 2, 1, 3, 0)))

        @pl.when(mq >= last)
        def _():
            finish(mq)

    for i in range(8):
        sent(x_rows(0, 0, PIECES[i + 2][2]), x_s.at[i])
    for f in range(2):
        for by in range(1, n):
            sent(w_dst(f, X), w1_s.at[f, by - 1])
        for i in range(4):
            sent(w_line(f, 0) if i < 2 else w_line(f, 0, 0, hn), w2_s.at[f, i])
            sent(w_line(f, 0), w3_s.at[f, i])
    for p in range(len(PIECES)):
        for kind, part in enumerate((k_part, k_part, v_part, v_part, k_part, v_part)):
            sent(part(p, PIECES[p][2], 0), kv_s.at[p, kind])

    pass_on()
    o2_finish(0)
    o2_forward(1)
    o2_finish(1)
    o_wait(0)
    o_wait(1)

    tn = 256

    def out_step(rels, final):
        lo = slots[rels[0]]

        @pl.loop(0, d // tn)
        def _(i):
            here = pl.ds(pl.multiple_of(i * tn, tn), tn)
            w = jnp.concatenate([wobuf[at(X, rel), :, :, :, here].reshape(width, tn) for rel in rels], axis=0)
            part = dot(seen[:, lo * width : (lo + len(rels)) * width], w, 1, 0)
            if final:
                yout[:, here] = (acc[:, here] + part).astype(y_ref.dtype)
                local(yout.at[:, here], y_ref.at[:, here], y_s.at[i])
            else:
                acc[:, here] = xbuf[X, :, here].astype(jnp.float32) + part

    got(seat(1), a_r.at[1])
    out_step((0, 1), False)
    got(seat(3), a_r.at[3])
    got(seat(2, 0, half), a_r.at[2])
    got(seat(2, half, half), a_r.at[0])
    out_step((3, 2), True)

    for o in range(2):
        for by in range(1, n):
            sent(o_block(o, 0), o1_s.at[o, by - 1])
        for i in range(4):
            sent(o_line(o, 0) if i < 2 else o_line(o, 0, 0, hn), o2_s.at[o, i])
            sent(o_line(o, 0), o3_s.at[o, i])
    for by in (1, -1):
        sent(sout.at[at(X, by)], a_s.at[at(X, by)])
    sent(relay, a_s.at[last])
    sent(relay, r_s.at[0])
    sent(relay, r_s.at[1])
    for i in range(d // tn):
        here = pl.ds(i * tn, tn)
        pltpu.make_async_copy(yout.at[:, here], y_ref.at[:, here], y_s.at[i]).wait()


def tables(own, chunks):
    half = HEAD // 2
    rate = np.float64(THETA) ** (-np.arange(half, dtype=np.float64) / half)
    row = np.arange(own, dtype=np.float64)[:, None] * rate
    chunk = (np.arange(chunks, dtype=np.float64) * own)[:, None] * rate
    return [f(t).astype(np.float32) for t in (row, chunk) for f in (np.cos, np.sin)]


def solution(mesh):
    n = math.isqrt(mesh.shape["sp"])

    def step(x, gain, wq, wk, wv, wo):
        own, d = x.shape
        g = wq.shape[1] // wk.shape[1]
        rows, orow = wq.shape[0], wo.shape[0] // 2
        cosr, sinr, cosc, sinc = tables(own, n * n)
        hbm, vmem = pl.BlockSpec(memory_space=pl.ANY), pl.BlockSpec(memory_space=pltpu.VMEM)
        bf, dma = jnp.bfloat16, pltpu.SemaphoreType.DMA
        return pl.pallas_call(
            functools.partial(kernel, n, g),
            out_shape=jax.ShapeDtypeStruct(x.shape, bf),
            in_specs=[hbm, vmem, hbm, hbm, hbm, hbm, vmem, vmem, vmem, vmem],
            out_specs=hbm,
            scratch_shapes=[
                pltpu.VMEM((n, own, d), bf),
                pltpu.VMEM((2, own // 2, d), bf),
                pltpu.VMEM((n, n, rows, 2 * g * HEAD), bf),
                pltpu.VMEM((n, n, 2, orow, d), bf),
                pltpu.VMEM((n, g * own, HEAD), bf),
                pltpu.VMEM((n, n, own, HEAD), bf),
                pltpu.VMEM((n, n, HEAD, own), bf),
                pltpu.VMEM((n, HEAD + 8, g * own), jnp.float32),
                pltpu.VMEM((n, 1, g * own), jnp.float32),
                pltpu.VMEM((n, own, g * HEAD), bf),
                pltpu.VMEM((own, n * g * HEAD), bf),
                pltpu.VMEM((own // 2, g * HEAD), bf),
                pltpu.VMEM((own, d), jnp.float32),
                pltpu.VMEM((own, d), bf),
                dma((8,)), dma((len(PIECES),)),
                dma((2, n - 1)), dma((2, n - 1)), dma((2,)),
                dma((2, 4)), dma((2, 4)), dma((2, 4)), dma((2, 4)),
                dma((2, n - 1)), dma((2, n - 1)), dma((2,)),
                dma((2, 4)), dma((2, 4)), dma((2, 4)), dma((2, 4)),
                dma((len(PIECES), 6)), dma((len(PIECES), 6)),
                dma((n,)), dma((n,)), dma((2,)), dma(()),
                dma((d // 256,)),
            ],
            compiler_params=pltpu.CompilerParams(collective_id=0, has_side_effects=True, vmem_limit_bytes=66_000_000),
        )(x, gain, wq, wk, wv, wo, cosr, sinr, cosc, sinc)

    tokens, whole = P(("dp", "sp"), None), P("sp", None)
    return jax.shard_map(
        step,
        mesh=mesh,
        in_specs=(tokens, P(None), whole, whole, whole, whole),
        out_specs=tokens,
        check_vma=False,
    )
```

```python
import functools
import math

import jax
import jax.numpy as jnp
import numpy as np
from jax import lax
from jax.experimental import pallas as pl
from jax.experimental.pallas import tpu as pltpu
from jax.sharding import PartitionSpec as P

HEAD = 256
THETA = 10000
NEG = -1e30
HIDDEN = 2 * NEG
LOG2E = 1.4426950408889634
MESH = pl.DeviceIdType.MESH

PIECES = ((0, 0, 2), (0, 2, 2), (-1, 0, 2), (1, 2, 2), (-1, 2, 2), (1, 0, 2), (2, 0, 1), (2, 2, 1), (2, 1, 1), (2, 3, 1))


def pick(t, values):
    out = jnp.int32(values[-1])
    for i in range(len(values) - 2, -1, -1):
        out = jnp.where(t == i, jnp.int32(values[i]), out)
    return out


def look(t, values):
    words = [sum(v << 2 * i for i, v in enumerate(values[at : at + 15])) for at in range(0, len(values), 15)]
    word = jnp.int32(words[-1])
    for i in range(len(words) - 2, -1, -1):
        word = jnp.where(t < 15 * (i + 1), jnp.int32(words[i]), word)
    return jnp.bitwise_and(lax.shift_right_logical(word, 2 * lax.rem(t, 15)), 3)


def dot(a, b, ca, cb):
    return lax.dot_general(a, b, (((ca,), (cb,)), ((), ())), preferred_element_type=jnp.float32)


def kernel(n, g, x_ref, gain_ref, wq_ref, wk_ref, wv_ref, wo_ref, cosr_ref, sinr_ref, cosc_ref, sinc_ref, y_ref,
           xbuf, xn, wbuf, wobuf, qbuf, kbuf, vbuf, mix, top, sout, seen, relay, acc, yout,
           x_s, x_r, w1_s, w1_r, w_l, w2_s, w2_r, w3_s, w3_r, o1_s, o1_r, o_l, o2_s, o2_r, o3_s, o3_r, kv_s, kv_r, a_s, a_r, r_s, r_r, y_s):
    own, d = x_ref.shape
    half, quarter = own // 2, own // 4
    rows = wq_ref.shape[0]
    orow = wo_ref.shape[0] // 2
    width = g * HEAD
    sp, dp = lax.axis_index("sp"), lax.axis_index("dp")
    X, Y = lax.div(sp, n), lax.rem(sp, n)
    c = lax.rem(dp, 2)
    partner = {"dp": dp + 1 - 2 * c}

    def at(v, by):
        return lax.rem(v + n + by, n)

    def on_x(by):
        return {"sp": at(X, by) * n + Y}

    def on_y(by):
        return {"sp": X * n + at(Y, by)}

    def send(src, dst, ss, rs, dev):
        pltpu.make_async_remote_copy(src_ref=src, dst_ref=dst, send_sem=ss, recv_sem=rs, device_id=dev, device_id_type=MESH).start()

    def got(dst, rs):
        pltpu.make_async_remote_copy(src_ref=dst, dst_ref=dst, send_sem=rs, recv_sem=rs, device_id=partner, device_id_type=MESH).wait_recv()

    def sent(src, ss):
        pltpu.make_async_remote_copy(src_ref=src, dst_ref=src, send_sem=ss, recv_sem=ss, device_id=partner, device_id_type=MESH).wait_send()

    def local(src, dst, sem):
        pltpu.make_async_copy(src, dst, sem).start()

    barrier = pltpu.get_barrier_semaphore()
    peers = [on_x(by) for by in range(1, n)] + [on_y(by) for by in range(1, n)] + [partner]
    for peer in peers:
        pl.semaphore_signal(barrier, inc=1, device_id=peer, device_id_type=MESH)
    pl.semaphore_wait(barrier, len(peers))

    def block(f, core):
        return pl.ds(pl.multiple_of((2 * f + core) * HEAD, HEAD), HEAD)

    def w_dst(f, xi):
        return wbuf.at[xi, Y, :, block(f, c)]

    def w_begin(f, src):
        for by in (1, n - 1, 2):
            send(src(at(X, by)), w_dst(f, X), w1_s.at[f, by - 1], w1_r.at[f, by - 1], on_x(by))
        local(src(X), w_dst(f, X), w_l.at[f])

    def head_of(ref):
        return lambda h: ref.at[:, pl.ds(pl.multiple_of(h * HEAD, HEAD), HEAD)]

    @pl.when(c == 0)
    def _():
        w_begin(0, head_of(wk_ref))

    @pl.when(c == 1)
    def _():
        w_begin(0, head_of(wv_ref))

    w_begin(1, lambda h: wq_ref.at[:, pl.ds(pl.multiple_of(h * width + c * HEAD, HEAD), HEAD)])

    def x_rows(by, lo, size):
        return xbuf.at[at(X, by), pl.ds(lo * quarter, size * quarter), :]

    for p in range(2):
        _, lo, size = PIECES[p]
        local(x_ref.at[pl.ds(lo * quarter, size * quarter), :], x_rows(0, lo, size), x_r.at[p])
    for i, p in enumerate((2, 3, 4, 5)):
        by, lo, size = PIECES[p]
        send(x_ref.at[pl.ds(lo * quarter, size * quarter), :], x_rows(0, lo, size), x_s.at[i], x_r.at[p], on_x(-by))

    def x_forward(p):
        by = PIECES[p][0]
        for k in (0, 2):
            _, lo, size = PIECES[p + 4 + k]
            send(x_rows(by, lo, size), x_rows(by, lo, size), x_s.at[p + 2 + k], x_r.at[p + 4 + k], on_x(-by))

    cut = d // (4 * 128) * 128

    def o_cols(o):
        return pl.ds(0, cut) if o == 0 else pl.ds(cut, d - cut)

    def o_first(o, by):
        return on_y(by) if o == 0 else on_x(by)

    def o_second(o, by):
        return on_x(by) if o == 0 else on_y(by)

    def o_block(o, by, lo=0, size=orow):
        xi, yi = (X, at(Y, by)) if o == 0 else (at(X, by), Y)
        return wobuf.at[xi, yi, c, pl.ds(lo, size), o_cols(o)]

    def o_line(o, by, lo=0, size=n, core=None):
        core = c if core is None else core
        if o == 0:
            return wobuf.at[at(X, by), pl.ds(lo, size), core, :, o_cols(o)]
        return wobuf.at[pl.ds(lo, size), at(Y, by), core, :, o_cols(o)]

    hr = orow // 2

    def o1_begin(o):
        src = wo_ref.at[pl.ds(pl.multiple_of(c * orow, orow), orow), o_cols(o)]
        send(src, o_block(o, 0), o1_s.at[o, 0], o1_r.at[o, 0], o_first(o, 1))
        send(src, o_block(o, 0), o1_s.at[o, 1], o1_r.at[o, 1], o_first(o, -1))
        local(src, o_block(o, 0), o_l.at[o])

    def o1_forward(o):
        got(o_block(o, -1), o1_r.at[o, 0])
        send(o_block(o, -1, 0, hr), o_block(o, -1, 0, hr), o1_s.at[o, 2], o1_r.at[o, 2], o_first(o, 1))
        got(o_block(o, 1), o1_r.at[o, 1])
        send(o_block(o, 1, hr, hr), o_block(o, 1, hr, hr), o1_s.at[o, 3], o1_r.at[o, 3], o_first(o, -1))

    def o3(o, k, by):
        send(o_line(o, by), o_line(o, by), o3_s.at[o, k], o3_r.at[o, k], partner)

    def o2_begin(o):
        got(o_block(o, 2, 0, hr), o1_r.at[o, 2])
        got(o_block(o, 2, hr, hr), o1_r.at[o, 3])
        pltpu.make_async_copy(o_block(o, 0), o_block(o, 0), o_l.at[o]).wait()
        send(o_line(o, 0), o_line(o, 0), o2_s.at[o, 0], o2_r.at[o, 0], o_second(o, 1))
        send(o_line(o, 0), o_line(o, 0), o2_s.at[o, 1], o2_r.at[o, 1], o_second(o, -1))
        o3(o, 0, 0)

    hn = n // 2

    def o2_forward(o):
        got(o_line(o, -1), o2_r.at[o, 0])
        send(o_line(o, -1, 0, hn), o_line(o, -1, 0, hn), o2_s.at[o, 2], o2_r.at[o, 2], o_second(o, 1))
        got(o_line(o, 1), o2_r.at[o, 1])
        send(o_line(o, 1, hn, hn), o_line(o, 1, hn, hn), o2_s.at[o, 3], o2_r.at[o, 3], o_second(o, -1))
        o3(o, 1, -1)
        o3(o, 2, 1)

    def o2_finish(o):
        got(o_line(o, 2, 0, hn), o2_r.at[o, 2])
        got(o_line(o, 2, hn, hn), o2_r.at[o, 3])
        o3(o, 3, 2)

    def o_wait(o):
        for k, by in enumerate((0, -1, 1, 2)):
            got(o_line(o, by, core=1 - c), o3_r.at[o, k])

    o1_begin(0)

    step = 32

    def piece_of(p):
        lo = pl.multiple_of(pick(p, [lo for _, lo, _ in PIECES]) * quarter, quarter)
        return at(X, pick(p, [by for by, _, _ in PIECES])), lo

    def norm(p, size):
        m, lo = piece_of(p)
        slot = lax.rem(p, 2)

        @pl.loop(0, size * quarter // step)
        def _(i):
            here = pl.ds(pl.multiple_of(i * step, step), step)
            t = xbuf[m, pl.ds(pl.multiple_of(lo + i * step, step), step), :].astype(jnp.float32)
            scale = lax.rsqrt(jnp.mean(t * t, -1, keepdims=True) + 1e-6)
            xn[slot, here, :] = (t * scale * gain_ref[...].astype(jnp.float32)[None, :]).astype(jnp.bfloat16)

    def columns(p, size, i):
        w = wbuf[:, :, :, i * HEAD : (i + 1) * HEAD].reshape(n * n * rows, HEAD)
        return dot(xn[lax.rem(p, 2), : size * quarter, :], w, 1, 0).astype(jnp.bfloat16)

    def turned(t, m, lo):
        place = m * n + Y
        cc, sc = cosc_ref[pl.ds(place, 1), :], sinc_ref[pl.ds(place, 1), :]
        cr, sr = cosr_ref[pl.ds(lo, t.shape[0]), :], sinr_ref[pl.ds(lo, t.shape[0]), :]
        cos, sin = cc * cr - sc * sr, sc * cr + cc * sr
        a, b = t[:, : HEAD // 2].astype(jnp.float32), t[:, HEAD // 2 :].astype(jnp.float32)
        return jnp.concatenate([a * cos - b * sin, b * cos + a * sin], -1).astype(jnp.bfloat16)

    def keys_values(p, size):
        m, lo = piece_of(p)
        kbuf[Y, m, pl.ds(lo, size * quarter), :] = turned(columns(p, size, 0), m, lo)
        vbuf[Y, m, :, pl.ds(lo, size * quarter)] = columns(p, size, 1).T

    def queries(p, size):
        m, lo = piece_of(p)
        for h in range(g):
            qbuf[m, pl.ds(pl.multiple_of(h * own + lo, quarter), size * quarter), :] = turned(columns(p, size, 2 + h), m, lo)

    def k_part(p, size, by):
        m, lo = piece_of(p)
        return kbuf.at[at(Y, by), m, pl.ds(lo, size * quarter), :]

    def v_part(p, size, by):
        m, lo = piece_of(p)
        return vbuf.at[at(Y, by), m, :, pl.ds(lo, size * quarter)]

    def kv_send(p, size):
        for kind, part, by in ((0, k_part, 1), (1, k_part, -1), (2, v_part, 1), (3, v_part, -1)):
            send(part(p, size, 0), part(p, size, 0), kv_s.at[p, kind], kv_r.at[p, kind], on_y(by))

    def kv_forward(*ps):
        for p in ps:
            k, v = k_part(p, PIECES[p][2], -1), v_part(p, PIECES[p][2], 1)
            got(k, kv_r.at[p, 0])
            send(k, k, kv_s.at[p, 4], kv_r.at[p, 4], on_y(1))
            got(v, kv_r.at[p, 3])
            send(v, v, kv_s.at[p, 5], kv_r.at[p, 5], on_y(-1))

    def kv_near(*ps):
        for p in ps:
            got(k_part(p, PIECES[p][2], 1), kv_r.at[p, 1])
            got(v_part(p, PIECES[p][2], -1), kv_r.at[p, 2])

    def kv_far(*ps):
        for p in ps:
            got(k_part(p, PIECES[p][2], 2), kv_r.at[p, 4])
            got(v_part(p, PIECES[p][2], 2), kv_r.at[p, 5])

    e = HEAD**-0.5 * LOG2E

    def tile(mq, j, mk, masked):
        keys = kbuf[j, mk]
        scores = [dot(keys, qbuf[mq, h * own : (h + 1) * own, :], 1, 1) for h in range(g)]
        weights, keeps = [], []
        for h, s in enumerate(scores):
            at_h = slice(h * own, (h + 1) * own)
            if masked:
                ok = lax.broadcasted_iota(jnp.int32, s.shape, 0) <= lax.broadcasted_iota(jnp.int32, s.shape, 1)
                s = jnp.where(ok, s, HIDDEN)
            old = top[mq, :, at_h]
            new = jnp.maximum(old, s.max(axis=0, keepdims=True))
            top[mq, :, at_h] = new
            weights.append(jnp.exp2((s - new) * e).astype(jnp.bfloat16))
            keeps.append(jnp.exp2((old - new) * e))
        values = jnp.concatenate([vbuf[j, mk], jnp.ones((8, own), jnp.bfloat16)], axis=0)
        for h in range(g):
            at_h = slice(h * own, (h + 1) * own)
            mix[mq, :, at_h] = mix[mq, :, at_h] * keeps[h] + dot(values, weights[h], 1, 0)

    def tile2(mq, j0, j1, mk):
        js = (j0, j1)
        scores = [[dot(kbuf[j, mk], qbuf[mq, h * own : (h + 1) * own, :], 1, 1) for j in js] for h in range(g)]
        weights, keeps = [], []
        for h, pair_ in enumerate(scores):
            at_h = slice(h * own, (h + 1) * own)
            old = top[mq, :, at_h]
            new = functools.reduce(jnp.maximum, [s.max(axis=0, keepdims=True) for s in pair_], old)
            top[mq, :, at_h] = new
            weights.append(jnp.concatenate([jnp.exp2((s - new) * e).astype(jnp.bfloat16) for s in pair_], axis=0))
            keeps.append(jnp.exp2((old - new) * e))
        values = jnp.concatenate([jnp.concatenate([vbuf[j, mk] for j in js], axis=1), jnp.ones((8, 2 * own), jnp.bfloat16)], axis=0)
        for h in range(g):
            at_h = slice(h * own, (h + 1) * own)
            mix[mq, :, at_h] = mix[mq, :, at_h] * keeps[h] + dot(values, weights[h], 1, 0)

    def later(ra, rb):
        ma, mb = at(X, ra), at(X, rb)
        return jnp.maximum(ma, mb), jnp.minimum(ma, mb)

    def singles(table, before=None):
        def body(t, _):
            for i, todo in (before or {}).items():

                @pl.when(t == i)
                def _(todo=todo):
                    todo()

            ra, rb, by = (look(t, [row[k] % n for row in table]) for k in range(3))
            (mq, mk), j = later(ra, rb), at(Y, by)
            q_place, k_place = mq * n + Y, mk * n + j

            @pl.when(k_place == q_place)
            def _():
                tile(mq, j, mk, True)

            @pl.when(k_place < q_place)
            def _():
                tile(mq, j, mk, False)

        lax.fori_loop(0, len(table), body, None)

    def cross(pairs, *places):
        return [(a, b, by) for by in places for a, b in pairs]

    last = at(X, 2)
    slots = (0, 2, 3, 1)

    def seat(rel, lo=0, size=own):
        return seen.at[pl.ds(lo, size), pl.ds(pl.multiple_of(pick(rel, slots) * width, width), width)]

    def finish(mq):
        out = mix[mq, :HEAD, :] * (1 / mix[mq, HEAD : HEAD + 1, :])
        to = at(mq, -X)
        back = at(X, -mq)
        for h in range(g):
            sout[mq, :, h * HEAD : (h + 1) * HEAD] = out[:, h * own : (h + 1) * own].T.astype(jnp.bfloat16)

        @pl.when(to == 0)
        def _():
            seen[:, :width] = sout[mq]

        @pl.when(to == 2)
        def _():
            send(sout.at[mq, pl.ds(half, half), :], relay, r_s.at[0], r_r, on_x(-1))
            send(sout.at[mq, pl.ds(0, half), :], seat(2, 0, half), a_s.at[mq], a_r.at[2], on_x(2))

        @pl.when((to == 1) | (to == 3))
        def _():
            send(sout.at[mq], seat(back), a_s.at[mq], a_r.at[back], {"sp": mq * n + Y})

    def pass_on():
        got(relay, r_r)
        send(relay, seat(2, half, half), r_s.at[1], a_r.at[0], on_x(-1))

    top[...] = jnp.full(top.shape, NEG, jnp.float32)

    @pl.loop(0, n)
    def _(m):
        mix[m] = jnp.zeros(mix.shape[1:], jnp.float32)

    def arrive(p, size):
        got(xbuf.at[0, pl.ds(0, size * quarter), :], x_r.at[p])

    def pair(a, size, f):
        lax.fori_loop(a, a + 2, lambda p, _: f(p, size), None)

    def early_half(p, size):
        norm(p, size)
        keys_values(p, size)
        kv_send(p, size)

    arrive(0, 2)
    arrive(1, 2)
    pair(0, 2, norm)

    def w_line(f, by, lo=0, size=n, core=None):
        return wbuf.at[pl.ds(lo, size), at(Y, by), :, block(f, c if core is None else core)]

    def w3(f, k, by):
        send(w_line(f, by), w_line(f, by), w3_s.at[f, k], w3_r.at[f, k], partner)

    def w2_begin(f):
        for by in range(1, n):
            got(w_dst(f, at(X, -by)), w1_r.at[f, by - 1])
        pltpu.make_async_copy(w_dst(f, X), w_dst(f, X), w_l.at[f]).wait()
        send(w_line(f, 0), w_line(f, 0), w2_s.at[f, 0], w2_r.at[f, 0], on_y(1))
        send(w_line(f, 0), w_line(f, 0), w2_s.at[f, 1], w2_r.at[f, 1], on_y(-1))
        w3(f, 0, 0)

    def w2_forward(f):
        got(w_line(f, -1), w2_r.at[f, 0])
        send(w_line(f, -1, 0, hn), w_line(f, -1, 0, hn), w2_s.at[f, 2], w2_r.at[f, 2], on_y(1))
        got(w_line(f, 1), w2_r.at[f, 1])
        send(w_line(f, 1, hn, hn), w_line(f, 1, hn, hn), w2_s.at[f, 3], w2_r.at[f, 3], on_y(-1))
        w3(f, 1, -1)
        w3(f, 2, 1)

    def w2_finish(f):
        got(w_line(f, 2, 0, hn), w2_r.at[f, 2])
        got(w_line(f, 2, hn, hn), w2_r.at[f, 3])
        w3(f, 3, 2)

    def w3_wait(f):
        for k, by in enumerate((0, -1, 1, 2)):
            got(w_line(f, by, core=1 - c), w3_r.at[f, k])

    w2_begin(0)
    o1_forward(0)
    w2_forward(0)
    w2_begin(1)
    w2_finish(0)
    w3_wait(0)
    pair(0, 2, keys_values)
    w2_forward(1)
    pair(0, 2, kv_send)
    w2_finish(1)
    w3_wait(1)
    pair(0, 2, queries)

    for p in (2, 3):
        arrive(p, 2)
        x_forward(p)
    pair(2, 2, early_half)
    kv_forward(0, 1)
    pair(2, 2, queries)
    o1_begin(1)
    singles(cross([(0, 0)], 0, 1, -1), {1: lambda: kv_near(0, 1)})
    kv_forward(2, 3)

    arrive(4, 2)
    arrive(5, 2)
    pair(4, 2, early_half)
    pair(4, 2, queries)
    pairs, same = [(0, -1), (0, 1), (-1, 1)], [(-1, -1), (1, 1)]
    singles(cross([(0, 0)], 2) + cross(pairs + same, 0), {0: lambda: kv_far(0, 1)})

    arrive(6, 1)
    arrive(7, 1)
    pair(6, 1, early_half)
    pair(6, 1, queries)
    kv_forward(4, 5)
    kv_near(2, 3, 4, 5)

    @pl.loop(0, len(pairs))
    def _(t):
        mq, mk = later(look(t, [a % n for a, _ in pairs]), look(t, [b % n for _, b in pairs]))
        tile2(mq, at(Y, 1), at(Y, -1), mk)

    singles(cross(same, 1, -1))
    kv_forward(6, 7)

    arrive(8, 1)
    arrive(9, 1)
    pair(8, 1, early_half)
    pair(8, 1, queries)

    o1_forward(1)
    o2_begin(0)
    kv_far(2, 3, 4, 5)
    singles(cross(pairs + same, 2))

    @pl.loop(0, n)
    def _(mq):
        @pl.when(mq < last)
        def _():
            finish(mq)

    kv_forward(8, 9)
    o2_begin(1)

    fourth = [(2, 0), (2, -1), (2, 1), (2, 2), (1, 2), (-1, 2), (0, 2)]

    def body(t, _):
        rq, rk = (look(t, [row[k] % n for row in fourth]) for k in range(2))
        mq, mk = at(X, rq), at(X, rk)

        @pl.when(t == 3)
        def _():
            o2_forward(0)
            kv_near(6, 7, 8, 9)
            kv_far(6, 7, 8, 9)

            @pl.loop(0, n)
            def _(j):
                @pl.when(j == Y)
                def _():
                    tile(mq, j, mk, True)

                @pl.when(j < Y)
                def _():
                    tile(mq, j, mk, False)

        @pl.when(mk < mq)
        def _():
            @pl.loop(0, 2)
            def _(i):
                tile2(mq, at(Y, 2 * i), at(Y, 2 * i + 1), mk)

        @pl.when((t >= 3) & (mq >= last))
        def _():
            finish(mq)

    lax.fori_loop(0, len(fourth), body, None)

    for i in range(8):
        sent(x_rows(0, 0, PIECES[i + 2][2]), x_s.at[i])
    for f in range(2):
        for by in range(1, n):
            sent(w_dst(f, X), w1_s.at[f, by - 1])
        for i in range(4):
            sent(w_line(f, 0) if i < 2 else w_line(f, 0, 0, hn), w2_s.at[f, i])
            sent(w_line(f, 0), w3_s.at[f, i])
    for p in range(len(PIECES)):
        for kind, part in enumerate((k_part, k_part, v_part, v_part, k_part, v_part)):
            sent(part(p, PIECES[p][2], 0), kv_s.at[p, kind])

    o2_forward(1)
    pass_on()
    o2_finish(0)
    o2_finish(1)
    o_wait(0)
    o_wait(1)

    tn = 256

    def out_step(rels, final):
        lo = slots[rels[0]]

        @pl.loop(0, d // tn)
        def _(i):
            here = pl.ds(pl.multiple_of(i * tn, tn), tn)
            w = jnp.concatenate([wobuf[at(X, rel), :, :, :, here].reshape(width, tn) for rel in rels], axis=0)
            part = dot(seen[:, lo * width : (lo + len(rels)) * width], w, 1, 0)
            if final:
                yout[:, here] = (acc[:, here] + part).astype(y_ref.dtype)
                local(yout.at[:, here], y_ref.at[:, here], y_s.at[i])
            else:
                acc[:, here] = xbuf[X, :, here].astype(jnp.float32) + part

    got(seat(3), a_r.at[3])
    out_step((0, 3), False)
    got(seat(1), a_r.at[1])
    got(seat(2, 0, half), a_r.at[2])
    got(seat(2, half, half), a_r.at[0])
    out_step((1, 2), True)

    for o in range(2):
        for i in range(4):
            sent(o_block(o, 0) if i < 2 else o_block(o, 0, 0, hr), o1_s.at[o, i])
            sent(o_line(o, 0) if i < 2 else o_line(o, 0, 0, hn), o2_s.at[o, i])
            sent(o_line(o, 0), o3_s.at[o, i])
    for by in (1, -1):
        sent(sout.at[at(X, by)], a_s.at[at(X, by)])
    sent(relay, a_s.at[last])
    sent(relay, r_s.at[0])
    sent(relay, r_s.at[1])
    for i in range(d // tn):
        here = pl.ds(i * tn, tn)
        pltpu.make_async_copy(yout.at[:, here], y_ref.at[:, here], y_s.at[i]).wait()


def tables(own, chunks):
    half = HEAD // 2
    rate = np.float64(THETA) ** (-np.arange(half, dtype=np.float64) / half)
    row = np.arange(own, dtype=np.float64)[:, None] * rate
    chunk = (np.arange(chunks, dtype=np.float64) * own)[:, None] * rate
    return [f(t).astype(np.float32) for t in (row, chunk) for f in (np.cos, np.sin)]


def solution(mesh):
    n = math.isqrt(mesh.shape["sp"])

    def step(x, gain, wq, wk, wv, wo):
        own, d = x.shape
        g = wq.shape[1] // wk.shape[1]
        rows, orow = wq.shape[0], wo.shape[0] // 2
        cosr, sinr, cosc, sinc = tables(own, n * n)
        hbm, vmem = pl.BlockSpec(memory_space=pl.ANY), pl.BlockSpec(memory_space=pltpu.VMEM)
        bf, dma = jnp.bfloat16, pltpu.SemaphoreType.DMA
        return pl.pallas_call(
            functools.partial(kernel, n, g),
            out_shape=jax.ShapeDtypeStruct(x.shape, bf),
            in_specs=[hbm, vmem, hbm, hbm, hbm, hbm, vmem, vmem, vmem, vmem],
            out_specs=hbm,
            scratch_shapes=[
                pltpu.VMEM((n, own, d), bf),
                pltpu.VMEM((2, own // 2, d), bf),
                pltpu.VMEM((n, n, rows, 2 * g * HEAD), bf),
                pltpu.VMEM((n, n, 2, orow, d), bf),
                pltpu.VMEM((n, g * own, HEAD), bf),
                pltpu.VMEM((n, n, own, HEAD), bf),
                pltpu.VMEM((n, n, HEAD, own), bf),
                pltpu.VMEM((n, HEAD + 8, g * own), jnp.float32),
                pltpu.VMEM((n, 1, g * own), jnp.float32),
                pltpu.VMEM((n, own, g * HEAD), bf),
                pltpu.VMEM((own, n * g * HEAD), bf),
                pltpu.VMEM((own // 2, g * HEAD), bf),
                pltpu.VMEM((own, d), jnp.float32),
                pltpu.VMEM((own, d), bf),
                dma((8,)), dma((len(PIECES),)),
                dma((2, n - 1)), dma((2, n - 1)), dma((2,)),
                dma((2, 4)), dma((2, 4)), dma((2, 4)), dma((2, 4)),
                dma((2, 4)), dma((2, 4)), dma((2,)),
                dma((2, 4)), dma((2, 4)), dma((2, 4)), dma((2, 4)),
                dma((len(PIECES), 6)), dma((len(PIECES), 6)),
                dma((n,)), dma((n,)), dma((2,)), dma(()),
                dma((d // 256,)),
            ],
            compiler_params=pltpu.CompilerParams(collective_id=0, has_side_effects=True, vmem_limit_bytes=66_000_000),
        )(x, gain, wq, wk, wv, wo, cosr, sinr, cosc, sinc)

    tokens, whole = P(("dp", "sp"), None), P("sp", None)
    return jax.shard_map(
        step,
        mesh=mesh,
        in_specs=(tokens, P(None), whole, whole, whole, whole),
        out_specs=tokens,
        check_vma=False,
    )
```

```python
import functools
import math

import jax
import jax.numpy as jnp
import numpy as np
from jax import lax
from jax.experimental import pallas as pl
from jax.experimental.pallas import tpu as pltpu
from jax.sharding import PartitionSpec as P

HEAD = 256
THETA = 10000
NEG = -1e30
HIDDEN = 2 * NEG
LOG2E = 1.4426950408889634
MESH = pl.DeviceIdType.MESH

PIECES = ((0, 0, 2), (0, 2, 2), (-1, 0, 2), (1, 2, 2), (-1, 2, 2), (1, 0, 2), (2, 0, 1), (2, 2, 1), (2, 1, 1), (2, 3, 1))


def pick(t, values):
    out = jnp.int32(values[-1])
    for i in range(len(values) - 2, -1, -1):
        out = jnp.where(t == i, jnp.int32(values[i]), out)
    return out


def look(t, values):
    words = [sum(v << 2 * i for i, v in enumerate(values[at : at + 15])) for at in range(0, len(values), 15)]
    word = jnp.int32(words[-1])
    for i in range(len(words) - 2, -1, -1):
        word = jnp.where(t < 15 * (i + 1), jnp.int32(words[i]), word)
    return jnp.bitwise_and(lax.shift_right_logical(word, 2 * lax.rem(t, 15)), 3)


def dot(a, b, ca, cb):
    return lax.dot_general(a, b, (((ca,), (cb,)), ((), ())), preferred_element_type=jnp.float32)


def kernel(n, g, x_ref, gain_hbm, wq_ref, wk_ref, wv_ref, wo_ref, angles_hbm, y_ref,
           gain_ref, angles, xbuf, xn, wbuf, wobuf, qbuf, kbuf, vbuf, mix, top, sout, seen, relay, acc, yout,
           c_l, x_s, x_r, w1_s, w1_r, w_l, w2_s, w2_r, w3_s, w3_r, o1_s, o1_r, o_l, o2_s, o2_r, o3_s, o3_r, kv_s, kv_pass, kv_near_r, kv_far_r,
           a_s, a_r, r_r, y_s):
    own, d = x_ref.shape
    half, quarter = own // 2, own // 4
    rows = wq_ref.shape[0]
    orow = wo_ref.shape[0] // 2
    width = g * HEAD
    sp, dp = lax.axis_index("sp"), lax.axis_index("dp")
    X, Y = lax.div(sp, n), lax.rem(sp, n)
    c = lax.rem(dp, 2)
    partner = {"dp": dp + 1 - 2 * c}

    def at(v, by):
        return lax.rem(v + n + by, n)

    def on_x(by):
        return {"sp": at(X, by) * n + Y}

    def on_y(by):
        return {"sp": X * n + at(Y, by)}

    def send(src, dst, ss, rs, dev):
        pltpu.make_async_remote_copy(src_ref=src, dst_ref=dst, send_sem=ss, recv_sem=rs, device_id=dev, device_id_type=MESH).start()

    def got(dst, rs):
        pltpu.make_async_remote_copy(src_ref=dst, dst_ref=dst, send_sem=rs, recv_sem=rs, device_id=partner, device_id_type=MESH).wait_recv()

    def sent(src, ss):
        pltpu.make_async_remote_copy(src_ref=src, dst_ref=src, send_sem=ss, recv_sem=ss, device_id=partner, device_id_type=MESH).wait_send()

    def local(src, dst, sem):
        pltpu.make_async_copy(src, dst, sem).start()

    local(gain_hbm, gain_ref, c_l.at[0])
    local(angles_hbm, angles, c_l.at[1])
    barrier = pltpu.get_barrier_semaphore()
    peers = [on_x(by) for by in range(1, n)] + [on_y(by) for by in range(1, n)] + [partner]
    for peer in peers:
        pl.semaphore_signal(barrier, inc=1, device_id=peer, device_id_type=MESH)
    pl.semaphore_wait(barrier, len(peers))

    def block(f, core):
        return pl.ds(pl.multiple_of((2 * f + core) * HEAD, HEAD), HEAD)

    def w_dst(f, xi):
        return wbuf.at[xi, Y, :, block(f, c)]

    def w_begin(f, src):
        for by in (1, n - 1, 2):
            send(src(at(X, by)), w_dst(f, X), w1_s, w1_r.at[f], on_x(by))
        local(src(X), w_dst(f, X), w_l.at[f])

    def head_of(ref):
        return lambda h: ref.at[:, pl.ds(pl.multiple_of(h * HEAD, HEAD), HEAD)]

    @pl.when(c == 0)
    def _():
        w_begin(0, head_of(wk_ref))

    @pl.when(c == 1)
    def _():
        w_begin(0, head_of(wv_ref))

    w_begin(1, lambda h: wq_ref.at[:, pl.ds(pl.multiple_of(h * width + c * HEAD, HEAD), HEAD)])

    def x_rows(by, lo, size):
        return xbuf.at[at(X, by), pl.ds(lo * quarter, size * quarter), :]

    for p in range(2):
        _, lo, size = PIECES[p]
        local(x_ref.at[pl.ds(lo * quarter, size * quarter), :], x_rows(0, lo, size), x_r.at[p])
    for p in (2, 3, 4, 5):
        by, lo, size = PIECES[p]
        send(x_ref.at[pl.ds(lo * quarter, size * quarter), :], x_rows(0, lo, size), x_s, x_r.at[p], on_x(-by))

    def x_forward(p):
        by = PIECES[p][0]
        for k in (0, 2):
            _, lo, size = PIECES[p + 4 + k]
            send(x_rows(by, lo, size), x_rows(by, lo, size), x_s, x_r.at[p + 4 + k], on_x(-by))

    cut = d // (3 * 128) * 128

    def o_cols(o):
        return pl.ds(0, cut) if o == 0 else pl.ds(cut, d - cut)

    def o_first(o, by):
        return on_y(by) if o == 0 else on_x(by)

    def o_second(o, by):
        return on_x(by) if o == 0 else on_y(by)

    def o_block(o, by, lo=0, size=orow):
        xi, yi = (X, at(Y, by)) if o == 0 else (at(X, by), Y)
        return wobuf.at[xi, yi, c, pl.ds(lo, size), o_cols(o)]

    def o_line(o, by, lo=0, size=n):
        if o == 0:
            return wobuf.at[at(X, by), pl.ds(lo, size), c, :, o_cols(o)]
        return wobuf.at[pl.ds(lo, size), at(Y, by), c, :, o_cols(o)]

    hr = orow // 2

    def o1_begin(o):
        src = wo_ref.at[pl.ds(pl.multiple_of(c * orow, orow), orow), o_cols(o)]
        send(src, o_block(o, 0), o1_s, o1_r.at[o, 0], o_first(o, 1))
        send(src, o_block(o, 0), o1_s, o1_r.at[o, 1], o_first(o, -1))
        local(src, o_block(o, 0), o_l.at[o])

    def o1_forward(o):
        got(o_block(o, -1), o1_r.at[o, 0])
        send(o_block(o, -1, 0, hr), o_block(o, -1, 0, hr), o1_s, o1_r.at[o, 2], o_first(o, 1))
        got(o_block(o, 1), o1_r.at[o, 1])
        send(o_block(o, 1, hr, hr), o_block(o, 1, hr, hr), o1_s, o1_r.at[o, 3], o_first(o, -1))

    def o3(o, by):
        send(o_line(o, by), o_line(o, by), o3_s, o3_r, partner)

    def o2_begin(o):
        got(o_block(o, 2, 0, hr), o1_r.at[o, 2])
        got(o_block(o, 2, hr, hr), o1_r.at[o, 3])
        pltpu.make_async_copy(o_block(o, 0), o_block(o, 0), o_l.at[o]).wait()
        send(o_line(o, 0), o_line(o, 0), o2_s, o2_r.at[o, 0], o_second(o, 1))
        send(o_line(o, 0), o_line(o, 0), o2_s, o2_r.at[o, 1], o_second(o, -1))
        o3(o, 0)

    hn = n // 2

    def o2_forward(o):
        got(o_line(o, -1), o2_r.at[o, 0])
        send(o_line(o, -1, 0, hn), o_line(o, -1, 0, hn), o2_s, o2_r.at[o, 2], o_second(o, 1))
        got(o_line(o, 1), o2_r.at[o, 1])
        send(o_line(o, 1, hn, hn), o_line(o, 1, hn, hn), o2_s, o2_r.at[o, 3], o_second(o, -1))
        o3(o, -1)
        o3(o, 1)

    def o2_finish(o):
        got(o_line(o, 2, 0, hn), o2_r.at[o, 2])
        got(o_line(o, 2, hn, hn), o2_r.at[o, 3])
        o3(o, 2)

    o1_begin(0)

    step = 32

    def piece_of(p):
        lo = pl.multiple_of(pick(p, [lo for _, lo, _ in PIECES]) * quarter, quarter)
        return at(X, pick(p, [by for by, _, _ in PIECES])), lo

    def norm(p, size):
        m, lo = piece_of(p)
        slot = lax.rem(p, 2)

        @pl.loop(0, size * quarter // step)
        def _(i):
            here = pl.ds(pl.multiple_of(i * step, step), step)
            t = xbuf[m, pl.ds(pl.multiple_of(lo + i * step, step), step), :].astype(jnp.float32)
            scale = lax.rsqrt(jnp.mean(t * t, -1, keepdims=True) + 1e-6)
            xn[slot, here, :] = (t * scale * gain_ref[...].astype(jnp.float32)[None, :]).astype(jnp.bfloat16)

    def columns(p, size, i):
        w = wbuf[:, :, :, i * HEAD : (i + 1) * HEAD].reshape(n * n * rows, HEAD)
        return dot(xn[lax.rem(p, 2), : size * quarter, :], w, 1, 0).astype(jnp.bfloat16)

    def turned(t, m, lo):
        place = m * n + Y
        cr, sr = (angles[pl.ds(f * own + lo, t.shape[0]), :] for f in range(2))
        cc, sc = (angles[pl.ds(2 * own + f * n * n + place, 1), :] for f in range(2))
        cos, sin = cc * cr - sc * sr, sc * cr + cc * sr
        a, b = t[:, : HEAD // 2].astype(jnp.float32), t[:, HEAD // 2 :].astype(jnp.float32)
        return jnp.concatenate([a * cos - b * sin, b * cos + a * sin], -1).astype(jnp.bfloat16)

    def keys_values(p, size):
        m, lo = piece_of(p)
        kbuf[Y, m, pl.ds(lo, size * quarter), :] = turned(columns(p, size, 0), m, lo)
        vbuf[Y, m, :, pl.ds(lo, size * quarter)] = columns(p, size, 1).T

    def queries(p, size):
        m, lo = piece_of(p)
        for h in range(g):
            qbuf[m, pl.ds(pl.multiple_of(h * own + lo, quarter), size * quarter), :] = turned(columns(p, size, 2 + h), m, lo)

    def k_part(p, size, by):
        m, lo = piece_of(p)
        return kbuf.at[at(Y, by), m, pl.ds(lo, size * quarter), :]

    def v_part(p, size, by):
        m, lo = piece_of(p)
        return vbuf.at[at(Y, by), m, :, pl.ds(lo, size * quarter)]

    def group(p):
        return jnp.where(p < 2, 0, jnp.where(p < 6, 1, 2))

    def kv_send(p, size):
        k, v = k_part(p, size, 0), v_part(p, size, 0)
        send(k, k, kv_s, kv_pass.at[p, 0], on_y(1))
        send(v, v, kv_s, kv_pass.at[p, 1], on_y(-1))
        send(k, k, kv_s, kv_near_r.at[group(p)], on_y(-1))
        send(v, v, kv_s, kv_near_r.at[group(p)], on_y(1))

    def kv_forward(*ps):
        for p in ps:
            k, v = k_part(p, PIECES[p][2], -1), v_part(p, PIECES[p][2], 1)
            got(k, kv_pass.at[p, 0])
            send(k, k, kv_s, kv_far_r.at[group(p)], on_y(1))
            got(v, kv_pass.at[p, 1])
            send(v, v, kv_s, kv_far_r.at[group(p)], on_y(-1))

    def kv_got(i, sem):
        got(kbuf.at[0, pl.ds(0, (2, 4, 2)[i])], sem.at[i])

    e = HEAD**-0.5 * LOG2E

    def tile(mq, j, mk, masked):
        keys = kbuf[j, mk]
        scores = [dot(keys, qbuf[mq, h * own : (h + 1) * own, :], 1, 1) for h in range(g)]
        weights, keeps = [], []
        for h, s in enumerate(scores):
            at_h = slice(h * own, (h + 1) * own)
            if masked:
                ok = lax.broadcasted_iota(jnp.int32, s.shape, 0) <= lax.broadcasted_iota(jnp.int32, s.shape, 1)
                s = jnp.where(ok, s, HIDDEN)
            old = top[mq, :, at_h]
            new = jnp.maximum(old, s.max(axis=0, keepdims=True))
            top[mq, :, at_h] = new
            weights.append(jnp.exp2((s - new) * e).astype(jnp.bfloat16))
            keeps.append(jnp.exp2((old - new) * e))
        values = jnp.concatenate([vbuf[j, mk], jnp.ones((8, own), jnp.bfloat16)], axis=0)
        for h in range(g):
            at_h = slice(h * own, (h + 1) * own)
            mix[mq, :, at_h] = mix[mq, :, at_h] * keeps[h] + dot(values, weights[h], 1, 0)

    def tile2(mq, j0, j1, mk):
        js = (j0, j1)
        scores = [[dot(kbuf[j, mk], qbuf[mq, h * own : (h + 1) * own, :], 1, 1) for j in js] for h in range(g)]
        weights, keeps = [], []
        for h, pair_ in enumerate(scores):
            at_h = slice(h * own, (h + 1) * own)
            old = top[mq, :, at_h]
            new = functools.reduce(jnp.maximum, [s.max(axis=0, keepdims=True) for s in pair_], old)
            top[mq, :, at_h] = new
            weights.append(jnp.concatenate([jnp.exp2((s - new) * e).astype(jnp.bfloat16) for s in pair_], axis=0))
            keeps.append(jnp.exp2((old - new) * e))
        values = jnp.concatenate([jnp.concatenate([vbuf[j, mk] for j in js], axis=1), jnp.ones((8, 2 * own), jnp.bfloat16)], axis=0)
        for h in range(g):
            at_h = slice(h * own, (h + 1) * own)
            mix[mq, :, at_h] = mix[mq, :, at_h] * keeps[h] + dot(values, weights[h], 1, 0)

    def later(ra, rb):
        ma, mb = at(X, ra), at(X, rb)
        return jnp.maximum(ma, mb), jnp.minimum(ma, mb)

    def singles(table, before=None):
        def body(t, _):
            for i, todo in (before or {}).items():

                @pl.when(t == i)
                def _(todo=todo):
                    todo()

            ra, rb, by = (look(t, [row[k] % n for row in table]) for k in range(3))
            (mq, mk), j = later(ra, rb), at(Y, by)
            q_place, k_place = mq * n + Y, mk * n + j

            @pl.when(k_place == q_place)
            def _():
                tile(mq, j, mk, True)

            @pl.when(k_place < q_place)
            def _():
                tile(mq, j, mk, False)

        lax.fori_loop(0, len(table), body, None)

    def cross(pairs, *places):
        return [(a, b, by) for by in places for a, b in pairs]

    last = at(X, 2)
    slots = (0, 2, 3, 1)

    def seat(rel, lo=0, size=own):
        return seen.at[pl.ds(lo, size), pl.ds(pl.multiple_of(pick(rel, slots) * width, width), width)]

    def finish(mq):
        out = mix[mq, :HEAD, :] * (1 / mix[mq, HEAD : HEAD + 1, :])
        to = at(mq, -X)
        back = at(X, -mq)
        for h in range(g):
            sout[mq, :, h * HEAD : (h + 1) * HEAD] = out[:, h * own : (h + 1) * own].T.astype(jnp.bfloat16)

        @pl.when(to == 0)
        def _():
            seen[:, :width] = sout[mq]

        @pl.when(to == 2)
        def _():
            send(sout.at[mq, pl.ds(half, half), :], relay, a_s, r_r, on_x(-1))
            send(sout.at[mq, pl.ds(0, half), :], seat(2, 0, half), a_s, a_r.at[2], on_x(2))

        @pl.when((to == 1) | (to == 3))
        def _():
            send(sout.at[mq], seat(back), a_s, a_r.at[back], {"sp": mq * n + Y})

    def pass_on():
        got(relay, r_r)
        send(relay, seat(2, half, half), a_s, a_r.at[0], on_x(-1))

    top[...] = jnp.full(top.shape, NEG, jnp.float32)

    @pl.loop(0, n)
    def _(m):
        mix[m] = jnp.zeros(mix.shape[1:], jnp.float32)

    def arrive(p, size):
        got(xbuf.at[0, pl.ds(0, size * quarter), :], x_r.at[p])

    def pair(a, size, f):
        lax.fori_loop(a, a + 2, lambda p, _: f(p, size), None)

    def early_half(p, size):
        norm(p, size)
        keys_values(p, size)
        kv_send(p, size)

    pltpu.make_async_copy(gain_hbm, gain_ref, c_l.at[0]).wait()
    pltpu.make_async_copy(angles_hbm, angles, c_l.at[1]).wait()
    arrive(0, 2)
    arrive(1, 2)
    pair(0, 2, norm)

    def w_line(f, by, lo=0, size=n):
        return wbuf.at[pl.ds(lo, size), at(Y, by), :, block(f, c)]

    def w3(f, by):
        send(w_line(f, by), w_line(f, by), w3_s, w3_r.at[f], partner)

    def w2_begin(f):
        got(wbuf.at[0, pl.ds(0, n - 1), :, pl.ds(0, HEAD)], w1_r.at[f])
        pltpu.make_async_copy(w_dst(f, X), w_dst(f, X), w_l.at[f]).wait()
        send(w_line(f, 0), w_line(f, 0), w2_s, w2_r.at[f, 0], on_y(1))
        send(w_line(f, 0), w_line(f, 0), w2_s, w2_r.at[f, 1], on_y(-1))
        w3(f, 0)

    def w2_forward(f):
        got(w_line(f, -1), w2_r.at[f, 0])
        send(w_line(f, -1, 0, hn), w_line(f, -1, 0, hn), w2_s, w2_r.at[f, 2], on_y(1))
        got(w_line(f, 1), w2_r.at[f, 1])
        send(w_line(f, 1, hn, hn), w_line(f, 1, hn, hn), w2_s, w2_r.at[f, 3], on_y(-1))
        w3(f, -1)
        w3(f, 1)

    def w2_finish(f):
        got(w_line(f, 2, 0, hn), w2_r.at[f, 2])
        got(w_line(f, 2, hn, hn), w2_r.at[f, 3])
        w3(f, 2)

    def w3_wait(f):
        got(wbuf.at[:, :, :, pl.ds(0, HEAD)], w3_r.at[f])

    w2_begin(0)
    o1_forward(0)
    w2_forward(0)
    w2_begin(1)
    w2_finish(0)
    w3_wait(0)
    pair(0, 2, keys_values)
    w2_forward(1)
    pair(0, 2, kv_send)
    w2_finish(1)
    w3_wait(1)
    pair(0, 2, queries)

    for p in (2, 3):
        arrive(p, 2)
        x_forward(p)
    pair(2, 2, early_half)
    kv_forward(0, 1)
    pair(2, 2, queries)
    o1_begin(1)
    singles(cross([(0, 0)], 0, 1, -1), {1: lambda: kv_got(0, kv_near_r)})
    kv_forward(2, 3)

    arrive(4, 2)
    arrive(5, 2)
    pair(4, 2, early_half)
    pair(4, 2, queries)
    pairs, same = [(0, -1), (0, 1), (-1, 1)], [(-1, -1), (1, 1)]
    singles(cross([(0, 0)], 2) + cross(pairs + same, 0), {0: lambda: kv_got(0, kv_far_r)})

    arrive(6, 1)
    arrive(7, 1)
    pair(6, 1, early_half)
    pair(6, 1, queries)
    kv_forward(4, 5)
    kv_got(1, kv_near_r)

    @pl.loop(0, len(pairs))
    def _(t):
        mq, mk = later(look(t, [a % n for a, _ in pairs]), look(t, [b % n for _, b in pairs]))
        tile2(mq, at(Y, 1), at(Y, -1), mk)

    singles(cross(same, 1, -1))
    kv_forward(6, 7)

    arrive(8, 1)
    arrive(9, 1)
    pair(8, 1, early_half)
    pair(8, 1, queries)

    o1_forward(1)
    o2_begin(0)
    kv_got(1, kv_far_r)
    singles(cross(pairs + same, 2))

    @pl.loop(0, n)
    def _(mq):
        @pl.when(mq < last)
        def _():
            finish(mq)

    kv_forward(8, 9)
    o2_begin(1)

    fourth = [(2, 0), (2, -1), (2, 1), (2, 2), (1, 2), (-1, 2), (0, 2)]

    def body(t, _):
        rq, rk = (look(t, [row[k] % n for row in fourth]) for k in range(2))
        mq, mk = at(X, rq), at(X, rk)

        @pl.when(t == 3)
        def _():
            o2_forward(0)
            kv_got(2, kv_near_r)
            kv_got(2, kv_far_r)

            @pl.loop(0, n)
            def _(j):
                @pl.when(j == Y)
                def _():
                    tile(mq, j, mk, True)

                @pl.when(j < Y)
                def _():
                    tile(mq, j, mk, False)

        @pl.when(mk < mq)
        def _():
            @pl.loop(0, 2)
            def _(i):
                tile2(mq, at(Y, 2 * i), at(Y, 2 * i + 1), mk)

        @pl.when((t >= 3) & (mq >= last))
        def _():
            finish(mq)

    lax.fori_loop(0, len(fourth), body, None)

    o2_forward(1)
    pass_on()
    o2_finish(0)
    o2_finish(1)
    got(wobuf.at[:, :, 0], o3_r)

    tn = 768

    def out_step(rels, final):
        lo = slots[rels[0]]

        @pl.loop(0, d // tn)
        def _(i):
            here = pl.ds(pl.multiple_of(i * tn, tn), tn)
            w = jnp.concatenate([wobuf[at(X, rel), :, :, :, here].reshape(width, tn) for rel in rels], axis=0)
            part = dot(seen[:, lo * width : (lo + len(rels)) * width], w, 1, 0)
            if final:
                yout[:, here] = (acc[:, here] + part).astype(y_ref.dtype)
                local(yout.at[:, here], y_ref.at[:, here], y_s)
            else:
                acc[:, here] = xbuf[X, :, here].astype(jnp.float32) + part

    got(seat(3), a_r.at[3])
    out_step((0, 3), False)
    got(seat(1), a_r.at[1])
    got(seat(2, 0, half), a_r.at[2])
    got(seat(2, half, half), a_r.at[0])
    out_step((1, 2), True)

    sent(xbuf.at[pl.ds(0, 3)], x_s)
    sent(wbuf.at[0, pl.ds(0, 3), :, pl.ds(0, 2 * HEAD)], w1_s)
    sent(wbuf.at[pl.ds(0, 3), :, :, pl.ds(0, 2 * HEAD)], w2_s)
    sent(wbuf.at[pl.ds(0, 2)], w3_s)
    sent(wobuf.at[0, pl.ds(0, 3), 0], o1_s)
    sent(wobuf.at[pl.ds(0, 3), :, 0], o2_s)
    sent(wobuf.at[:, :, 0], o3_s)
    sent(xbuf.at[:, :, pl.ds(0, 6 * HEAD)], kv_s)
    sent(sout.at[:, pl.ds(0, own * 7 // 8)], a_s)
    pltpu.make_async_copy(yout, y_ref, y_s).wait()


def tables(own, chunks):
    half = HEAD // 2
    rate = np.float64(THETA) ** (-np.arange(half, dtype=np.float64) / half)
    row = np.arange(own, dtype=np.float64)[:, None] * rate
    chunk = (np.arange(chunks, dtype=np.float64) * own)[:, None] * rate
    return np.concatenate([f(t) for t in (row, chunk) for f in (np.cos, np.sin)]).astype(np.float32)


def solution(mesh):
    n = math.isqrt(mesh.shape["sp"])

    def step(x, gain, wq, wk, wv, wo):
        own, d = x.shape
        g = wq.shape[1] // wk.shape[1]
        rows, orow = wq.shape[0], wo.shape[0] // 2
        angles = tables(own, n * n)
        hbm = pl.BlockSpec(memory_space=pl.ANY)
        bf, dma = jnp.bfloat16, pltpu.SemaphoreType.DMA
        return pl.pallas_call(
            functools.partial(kernel, n, g),
            out_shape=jax.ShapeDtypeStruct(x.shape, bf),
            in_specs=[hbm] * 7,
            out_specs=hbm,
            scratch_shapes=[
                pltpu.VMEM(gain.shape, bf),
                pltpu.VMEM(angles.shape, jnp.float32),
                pltpu.VMEM((n, own, d), bf),
                pltpu.VMEM((2, own // 2, d), bf),
                pltpu.VMEM((n, n, rows, 2 * g * HEAD), bf),
                pltpu.VMEM((n, n, 2, orow, d), bf),
                pltpu.VMEM((n, g * own, HEAD), bf),
                pltpu.VMEM((n, n, own, HEAD), bf),
                pltpu.VMEM((n, n, HEAD, own), bf),
                pltpu.VMEM((n, HEAD + 8, g * own), jnp.float32),
                pltpu.VMEM((n, 1, g * own), jnp.float32),
                pltpu.VMEM((n, own, g * HEAD), bf),
                pltpu.VMEM((own, n * g * HEAD), bf),
                pltpu.VMEM((own // 2, g * HEAD), bf),
                pltpu.VMEM((own, d), jnp.float32),
                pltpu.VMEM((own, d), bf),
                dma((2,)),
                dma(()), dma((len(PIECES),)),
                dma(()), dma((2,)), dma((2,)),
                dma(()), dma((2, 4)), dma(()), dma((2,)),
                dma(()), dma((2, 4)), dma((2,)),
                dma(()), dma((2, 4)), dma(()), dma(()),
                dma(()), dma((len(PIECES), 2)), dma((3,)), dma((3,)),
                dma(()), dma((n,)), dma(()),
                dma(()),
            ],
            compiler_params=pltpu.CompilerParams(collective_id=0, has_side_effects=True, vmem_limit_bytes=66_000_000),
        )(x, gain, wq, wk, wv, wo, angles)

    tokens, whole = P(("dp", "sp"), None), P("sp", None)
    return jax.shard_map(
        step,
        mesh=mesh,
        in_specs=(tokens, P(None), whole, whole, whole, whole),
        out_specs=tokens,
        check_vma=False,
    )
```

```python
import functools
import math

import jax
import jax.numpy as jnp
import numpy as np
from jax import lax
from jax.experimental import pallas as pl
from jax.experimental.pallas import tpu as pltpu
from jax.sharding import PartitionSpec as P

HEAD = 256
THETA = 10000
NEG = -1e30
HIDDEN = 2 * NEG
LOG2E = 1.4426950408889634
MESH = pl.DeviceIdType.MESH
LEFT, OWN, RIGHT, FAR = -1, 0, 1, 2

PIECES = (*((by, 2 * h, 2) for by, h in ((OWN, OWN), (OWN, RIGHT), (LEFT, OWN), (RIGHT, RIGHT), (LEFT, RIGHT), (RIGHT, OWN))), *((FAR, lo, 1) for lo in (0, 2, 1, 3)))


def upto(size):
    return pl.ds(0, size)


def pick(t, values):
    out = jnp.int32(values[-1])
    for i in range(len(values) - 2, -1, -1):
        out = jnp.where(t == i, jnp.int32(values[i]), out)
    return out


def look(t, values):
    words = [sum(v << 2 * i for i, v in enumerate(values[at : at + 15])) for at in range(0, len(values), 15)]
    word = jnp.int32(words[-1])
    for i in range(len(words) - 2, -1, -1):
        word = jnp.where(t < 15 * (i + 1), jnp.int32(words[i]), word)
    return jnp.bitwise_and(lax.shift_right_logical(word, 2 * lax.rem(t, 15)), 3)


def dot(a, b, cb=0):
    return lax.dot_general(a, b, (((1,), (cb,)), ((), ())), preferred_element_type=jnp.float32)


def kernel(n, g, x_ref, gain_hbm, wq_ref, wk_ref, wv_ref, wo_ref, angles_hbm, y_ref,
           gain_ref, angles, xbuf, xn, wbuf, wobuf, qbuf, kbuf, vbuf, mix, top, sout, seen, relay, acc, yout,
           c_l, x_s, x_r, w1_s, w1_r, w_l, w2_s, w2_r, w3_s, w3_r, o1_s, o1_r, o_l, o2_s, o2_r, o3_s, o3_r, kv_s, kv_pass, kv_near_r, kv_far_r,
           a_s, a_r, r_r, y_s):
    own, d = x_ref.shape
    half, quarter = own // 2, own // 4
    rows = wq_ref.shape[0]
    orow = wo_ref.shape[0] // 2
    width = g * HEAD
    sp, dp = lax.axis_index("sp"), lax.axis_index("dp")
    X, Y = lax.div(sp, n), lax.rem(sp, n)
    c = lax.rem(dp, 2)
    partner = {"dp": dp + 1 - 2 * c}

    def at(v, by):
        return lax.rem(v + n + by, n)

    def on_x(by):
        return {"sp": at(X, by) * n + Y}

    def on_y(by):
        return {"sp": X * n + at(Y, by)}

    def send(src, dst, ss, rs, dev):
        pltpu.make_async_remote_copy(src_ref=src, dst_ref=dst, send_sem=ss, recv_sem=rs, device_id=dev, device_id_type=MESH).start()

    def got(dst, rs):
        pltpu.make_async_remote_copy(src_ref=dst, dst_ref=dst, send_sem=rs, recv_sem=rs, device_id=partner, device_id_type=MESH).wait_recv()

    def sent(src, ss):
        pltpu.make_async_remote_copy(src_ref=src, dst_ref=src, send_sem=ss, recv_sem=ss, device_id=partner, device_id_type=MESH).wait_send()

    def local(src, dst, sem):
        pltpu.make_async_copy(src, dst, sem).start()

    local(gain_hbm, gain_ref, c_l.at[0])
    local(angles_hbm, angles, c_l.at[1])
    barrier = pltpu.get_barrier_semaphore()
    peers = [on_x(by) for by in range(1, n)] + [on_y(by) for by in range(1, n)] + [partner]
    for peer in peers:
        pl.semaphore_signal(barrier, inc=1, device_id=peer, device_id_type=MESH)
    pl.semaphore_wait(barrier, len(peers))

    def block(f, core):
        return pl.ds(pl.multiple_of((2 * f + core) * HEAD, HEAD), HEAD)

    def w_dst(f, xi):
        return wbuf.at[xi, Y, :, block(f, c)]

    def w_begin(f, src):
        for by in (1, n - 1, 2):
            send(src(at(X, by)), w_dst(f, X), w1_s, w1_r.at[f], on_x(by))
        local(src(X), w_dst(f, X), w_l.at[f])

    def head_of(ref):
        return lambda h: ref.at[:, pl.ds(pl.multiple_of(h * HEAD, HEAD), HEAD)]

    @pl.when(c == 0)
    def _():
        w_begin(0, head_of(wk_ref))

    @pl.when(c == 1)
    def _():
        w_begin(0, head_of(wv_ref))

    w_begin(1, lambda h: wq_ref.at[:, pl.ds(pl.multiple_of(h * width + c * HEAD, HEAD), HEAD)])

    def x_rows(by, lo, size):
        return xbuf.at[at(X, by), pl.ds(lo * quarter, size * quarter), :]

    for p in range(2):
        _, lo, size = PIECES[p]
        local(x_ref.at[pl.ds(lo * quarter, size * quarter), :], x_rows(0, lo, size), x_r.at[p])
    for p in (2, 3, 4, 5):
        by, lo, size = PIECES[p]
        send(x_ref.at[pl.ds(lo * quarter, size * quarter), :], x_rows(0, lo, size), x_s, x_r.at[p], on_x(-by))

    def x_forward(p):
        by = PIECES[p][0]
        for k in (0, 2):
            _, lo, size = PIECES[p + 4 + k]
            send(x_rows(by, lo, size), x_rows(by, lo, size), x_s, x_r.at[p + 4 + k], on_x(-by))

    cut = d // (3 * 128) * 128

    def o_cols(o):
        return upto(cut) if o == 0 else pl.ds(cut, d - cut)

    def o_first(o, by):
        return on_y(by) if o == 0 else on_x(by)

    def o_second(o, by):
        return on_x(by) if o == 0 else on_y(by)

    def o_block(o, by, lo=0, size=orow):
        xi, yi = (X, at(Y, by)) if o == 0 else (at(X, by), Y)
        return wobuf.at[xi, yi, c, pl.ds(lo, size), o_cols(o)]

    def o_line(o, by, lo=0, size=n):
        if o == 0:
            return wobuf.at[at(X, by), pl.ds(lo, size), c, :, o_cols(o)]
        return wobuf.at[pl.ds(lo, size), at(Y, by), c, :, o_cols(o)]

    hr, hn = orow // 2, n // 2

    def o1_begin(o):
        src = wo_ref.at[pl.ds(pl.multiple_of(c * orow, orow), orow), o_cols(o)]
        send(src, o_block(o, OWN), o1_s, o1_r.at[o, 0], o_first(o, RIGHT))
        send(src, o_block(o, OWN), o1_s, o1_r.at[o, 1], o_first(o, LEFT))
        local(src, o_block(o, OWN), o_l.at[o])

    def o1_forward(o):
        got(o_block(o, LEFT), o1_r.at[o, 0])
        send(o_block(o, LEFT, 0, hr), o_block(o, LEFT, 0, hr), o1_s, o1_r.at[o, 2], o_first(o, RIGHT))
        got(o_block(o, RIGHT), o1_r.at[o, 1])
        send(o_block(o, RIGHT, hr, hr), o_block(o, RIGHT, hr, hr), o1_s, o1_r.at[o, 3], o_first(o, LEFT))

    def o3(o, by):
        send(o_line(o, by), o_line(o, by), o3_s, o3_r, partner)

    def o2_begin(o):
        got(o_block(o, FAR, 0, hr), o1_r.at[o, 2])
        got(o_block(o, FAR, hr, hr), o1_r.at[o, 3])
        pltpu.make_async_copy(o_block(o, OWN), o_block(o, OWN), o_l.at[o]).wait()
        for k, lo in ((0, 0), (1, hn)):
            send(o_line(o, OWN, lo, hn), o_line(o, OWN, lo, hn), o2_s, o2_r.at[o, k], o_second(o, RIGHT))
        for k, lo in ((2, hn), (3, 0)):
            send(o_line(o, OWN, lo, hn), o_line(o, OWN, lo, hn), o2_s, o2_r.at[o, k], o_second(o, LEFT))
        o3(o, OWN)

    def o2_forward(o):
        got(o_line(o, LEFT, 0, hn), o2_r.at[o, 0])
        send(o_line(o, LEFT, 0, hn), o_line(o, LEFT, 0, hn), o2_s, o2_r.at[o, 4], o_second(o, RIGHT))
        got(o_line(o, RIGHT, hn, hn), o2_r.at[o, 2])
        send(o_line(o, RIGHT, hn, hn), o_line(o, RIGHT, hn, hn), o2_s, o2_r.at[o, 5], o_second(o, LEFT))

    def o2_near(o):
        got(o_line(o, LEFT, hn, hn), o2_r.at[o, 1])
        o3(o, LEFT)
        got(o_line(o, RIGHT, 0, hn), o2_r.at[o, 3])
        o3(o, RIGHT)

    def o2_finish(o):
        got(o_line(o, FAR, 0, hn), o2_r.at[o, 4])
        got(o_line(o, FAR, hn, hn), o2_r.at[o, 5])
        o3(o, FAR)

    o1_begin(0)

    step = 32

    def piece_of(p):
        lo = pl.multiple_of(pick(p, [lo for _, lo, _ in PIECES]) * quarter, quarter)
        return at(X, pick(p, [by for by, _, _ in PIECES])), lo

    def norm(p, size):
        m, lo = piece_of(p)
        slot = lax.rem(p, 2)

        @pl.loop(0, size * quarter // step)
        def _(i):
            here = pl.ds(pl.multiple_of(i * step, step), step)
            t = xbuf[m, pl.ds(pl.multiple_of(lo + i * step, step), step), :].astype(jnp.float32)
            scale = lax.rsqrt(jnp.mean(t * t, -1, keepdims=True) + 1e-6)
            xn[slot, here, :] = (t * scale * gain_ref[...].astype(jnp.float32)[None, :]).astype(jnp.bfloat16)

    def columns(p, size, i):
        w = wbuf[:, :, :, i * HEAD : (i + 1) * HEAD].reshape(n * n * rows, HEAD)
        return dot(xn[lax.rem(p, 2), : size * quarter, :], w).astype(jnp.bfloat16)

    def turned(t, m, lo):
        place = m * n + Y
        cr, sr = (angles[pl.ds(f * own + lo, t.shape[0]), :] for f in range(2))
        cc, sc = (angles[pl.ds(2 * own + f * n * n + place, 1), :] for f in range(2))
        cos, sin = cc * cr - sc * sr, sc * cr + cc * sr
        a, b = t[:, : HEAD // 2].astype(jnp.float32), t[:, HEAD // 2 :].astype(jnp.float32)
        return jnp.concatenate([a * cos - b * sin, b * cos + a * sin], -1).astype(jnp.bfloat16)

    def keys_values(p, size):
        m, lo = piece_of(p)
        kbuf[Y, m, pl.ds(lo, size * quarter), :] = turned(columns(p, size, 0), m, lo)
        vbuf[Y, m, :, pl.ds(lo, size * quarter)] = columns(p, size, 1).T

    def queries(p, size):
        m, lo = piece_of(p)
        for h in range(g):
            qbuf[m, pl.ds(pl.multiple_of(h * own + lo, quarter), size * quarter), :] = turned(columns(p, size, 2 + h), m, lo)

    def k_part(p, size, by):
        m, lo = piece_of(p)
        return kbuf.at[at(Y, by), m, pl.ds(lo, size * quarter), :]

    def v_part(p, size, by):
        m, lo = piece_of(p)
        return vbuf.at[at(Y, by), m, :, pl.ds(lo, size * quarter)]

    def group(p):
        return jnp.where(p < 2, 0, jnp.where(p < 6, 1, 2))

    def kv_send(p, size):
        k, v = k_part(p, size, 0), v_part(p, size, 0)
        send(k, k, kv_s, kv_pass.at[p, 0], on_y(RIGHT))
        send(v, v, kv_s, kv_pass.at[p, 1], on_y(LEFT))
        send(k, k, kv_s, kv_near_r.at[group(p)], on_y(LEFT))
        send(v, v, kv_s, kv_near_r.at[group(p)], on_y(RIGHT))

    def kv_forward(*ps):
        for p in ps:
            k, v = k_part(p, PIECES[p][2], -1), v_part(p, PIECES[p][2], 1)
            got(k, kv_pass.at[p, 0])
            send(k, k, kv_s, kv_far_r.at[group(p)], on_y(RIGHT))
            got(v, kv_pass.at[p, 1])
            send(v, v, kv_s, kv_far_r.at[group(p)], on_y(LEFT))

    def kv_got(i, sem):
        got(kbuf.at[0, upto((2, 4, 2)[i])], sem.at[i])

    e = HEAD**-0.5 * LOG2E

    def heads(h):
        return slice(h * own, (h + 1) * own)

    def tile(mq, j, mk, masked):
        keys = kbuf[j, mk]
        scores = [dot(keys, qbuf[mq, heads(h), :], 1) for h in range(g)]
        weights, keeps = [], []
        for h, s in enumerate(scores):
            at_h = heads(h)
            if masked:
                ok = lax.broadcasted_iota(jnp.int32, s.shape, 0) <= lax.broadcasted_iota(jnp.int32, s.shape, 1)
                s = jnp.where(ok, s, HIDDEN)
            old = top[mq, :, at_h]
            new = jnp.maximum(old, s.max(axis=0, keepdims=True))
            top[mq, :, at_h] = new
            weights.append(jnp.exp2((s - new) * e).astype(jnp.bfloat16))
            keeps.append(jnp.exp2((old - new) * e))
        values = jnp.concatenate([vbuf[j, mk], jnp.ones((8, own), jnp.bfloat16)], axis=0)
        for h in range(g):
            at_h = heads(h)
            mix[mq, :, at_h] = mix[mq, :, at_h] * keeps[h] + dot(values, weights[h])

    def tile2(mq, j0, j1, mk):
        js = (j0, j1)
        scores = [[dot(kbuf[j, mk], qbuf[mq, heads(h), :], 1) for j in js] for h in range(g)]
        weights, keeps = [], []
        for h, pair_ in enumerate(scores):
            at_h = heads(h)
            old = top[mq, :, at_h]
            new = functools.reduce(jnp.maximum, [s.max(axis=0, keepdims=True) for s in pair_], old)
            top[mq, :, at_h] = new
            weights.append(jnp.concatenate([jnp.exp2((s - new) * e).astype(jnp.bfloat16) for s in pair_], axis=0))
            keeps.append(jnp.exp2((old - new) * e))
        values = jnp.concatenate([jnp.concatenate([vbuf[j, mk] for j in js], axis=1), jnp.ones((8, 2 * own), jnp.bfloat16)], axis=0)
        for h in range(g):
            at_h = heads(h)
            mix[mq, :, at_h] = mix[mq, :, at_h] * keeps[h] + dot(values, weights[h])

    def later(ra, rb):
        ma, mb = at(X, ra), at(X, rb)
        return jnp.maximum(ma, mb), jnp.minimum(ma, mb)

    def singles(table, before=None):
        def body(t, _):
            for i, todo in (before or {}).items():

                @pl.when(t == i)
                def _(todo=todo):
                    todo()

            ra, rb, by = (look(t, [row[k] % n for row in table]) for k in range(3))
            (mq, mk), j = later(ra, rb), at(Y, by)
            q_place, k_place = mq * n + Y, mk * n + j

            @pl.when(k_place == q_place)
            def _():
                tile(mq, j, mk, True)

            @pl.when(k_place < q_place)
            def _():
                tile(mq, j, mk, False)

        lax.fori_loop(0, len(table), body, None)

    def cross(pairs, *places):
        return [(a, b, by) for by in places for a, b in pairs]

    last = at(X, FAR)
    slots = (0, 2, 3, 1)

    def seat(rel, lo=0, size=own):
        return seen.at[pl.ds(lo, size), pl.ds(pl.multiple_of(pick(rel, slots) * width, width), width)]

    part = own // 8 * 3 // 2
    kept = own - 2 * part

    def finish(mq):
        out = mix[mq, :HEAD, :] * (1 / mix[mq, HEAD : HEAD + 1, :])
        to = at(mq, -X)
        back = at(X, -mq)
        for h in range(g):
            sout[mq, :, h * HEAD : (h + 1) * HEAD] = out[:, heads(h)].T.astype(jnp.bfloat16)

        @pl.when(to == 0)
        def _():
            seen[:, :width] = sout[mq]

        @pl.when(to == 2)
        def _():
            for i in range(2):
                send(sout.at[mq, pl.ds(kept + i * part, part), :], relay.at[i], a_s, r_r.at[i], on_x(LEFT))
            send(sout.at[mq, upto(kept), :], seat(FAR, 0, kept), a_s, a_r.at[2], on_x(FAR))

        @pl.when((to == 1) | (to == 3))
        def _():
            send(sout.at[mq], seat(back), a_s, a_r.at[back], {"sp": mq * n + Y})

    def pass_on():
        for i in range(2):
            got(relay.at[i], r_r.at[i])
            send(relay.at[i], seat(FAR, kept + i * part, part), a_s, a_r.at[0], on_x(LEFT))

    top[...] = jnp.full(top.shape, NEG, jnp.float32)

    @pl.loop(0, n)
    def _(m):
        mix[m] = jnp.zeros(mix.shape[1:], jnp.float32)

    def arrive(p, size):
        got(xbuf.at[0, upto(size * quarter), :], x_r.at[p])

    def pair(a, size, f):
        lax.fori_loop(a, a + 2, lambda p, _: f(p, size), None)

    def early_half(p, size):
        norm(p, size)
        keys_values(p, size)
        kv_send(p, size)

    pltpu.make_async_copy(gain_hbm, gain_ref, c_l.at[0]).wait()
    pltpu.make_async_copy(angles_hbm, angles, c_l.at[1]).wait()
    arrive(0, 2)
    arrive(1, 2)
    pair(0, 2, norm)

    def w_line(f, by, lo=0, size=n):
        return wbuf.at[pl.ds(lo, size), at(Y, by), :, block(f, c)]

    def w3(f, by):
        send(w_line(f, by), w_line(f, by), w3_s, w3_r.at[f], partner)

    def w2_begin(f):
        got(wbuf.at[0, upto(n - 1), :, upto(HEAD)], w1_r.at[f])
        pltpu.make_async_copy(w_dst(f, X), w_dst(f, X), w_l.at[f]).wait()
        send(w_line(f, OWN), w_line(f, OWN), w2_s, w2_r.at[f, 0], on_y(RIGHT))
        send(w_line(f, OWN), w_line(f, OWN), w2_s, w2_r.at[f, 1], on_y(LEFT))
        w3(f, OWN)

    def w2_forward(f):
        got(w_line(f, LEFT), w2_r.at[f, 0])
        send(w_line(f, LEFT, 0, hn), w_line(f, LEFT, 0, hn), w2_s, w2_r.at[f, 2], on_y(RIGHT))
        got(w_line(f, RIGHT), w2_r.at[f, 1])
        send(w_line(f, RIGHT, hn, hn), w_line(f, RIGHT, hn, hn), w2_s, w2_r.at[f, 3], on_y(LEFT))
        w3(f, LEFT)
        w3(f, RIGHT)

    def w2_finish(f):
        got(w_line(f, FAR, 0, hn), w2_r.at[f, 2])
        got(w_line(f, FAR, hn, hn), w2_r.at[f, 3])
        w3(f, FAR)

    def w3_wait(f):
        got(wbuf.at[:, :, :, upto(HEAD)], w3_r.at[f])

    w2_begin(0)
    o1_forward(0)
    w2_forward(0)
    w2_begin(1)
    w2_finish(0)
    w3_wait(0)
    pair(0, 2, keys_values)
    w2_forward(1)
    pair(0, 2, kv_send)
    w2_finish(1)
    w3_wait(1)
    pair(0, 2, queries)

    for p in (2, 3):
        arrive(p, 2)
        x_forward(p)
    pair(2, 2, early_half)
    kv_forward(0, 1)
    pair(2, 2, queries)
    o1_begin(1)
    singles(cross([(OWN, OWN)], OWN, RIGHT, LEFT), {1: lambda: kv_got(0, kv_near_r)})
    kv_forward(2, 3)

    arrive(4, 2)
    arrive(5, 2)
    pair(4, 2, early_half)
    pair(4, 2, queries)
    pairs, same = [(OWN, LEFT), (OWN, RIGHT), (LEFT, RIGHT)], [(LEFT, LEFT), (RIGHT, RIGHT)]
    singles(cross([(OWN, OWN)], FAR) + cross(pairs + same, OWN), {0: lambda: kv_got(0, kv_far_r)})

    arrive(6, 1)
    arrive(7, 1)
    pair(6, 1, early_half)
    pair(6, 1, queries)
    kv_forward(4, 5)
    kv_got(1, kv_near_r)

    @pl.loop(0, len(pairs))
    def _(t):
        mq, mk = later(look(t, [a % n for a, _ in pairs]), look(t, [b % n for _, b in pairs]))
        tile2(mq, at(Y, RIGHT), at(Y, LEFT), mk)

    singles(cross(same, RIGHT, LEFT))
    kv_forward(6, 7)

    arrive(8, 1)
    arrive(9, 1)
    pair(8, 1, early_half)
    pair(8, 1, queries)

    o1_forward(1)
    o2_begin(0)
    kv_got(1, kv_far_r)
    singles(cross(pairs + same, FAR))

    @pl.loop(0, n)
    def _(mq):
        @pl.when(mq < last)
        def _():
            finish(mq)

    kv_forward(8, 9)
    o2_begin(1)

    fourth = [*((FAR, by) for by in (OWN, LEFT, RIGHT, FAR)), *((by, FAR) for by in (RIGHT, LEFT, OWN))]

    def body(t, _):
        rq, rk = (look(t, [row[k] % n for row in fourth]) for k in range(2))
        mq, mk = at(X, rq), at(X, rk)

        @pl.when(t == 3)
        def _():
            o2_forward(0)
            kv_got(2, kv_near_r)
            kv_got(2, kv_far_r)

            @pl.loop(0, n)
            def _(j):
                @pl.when(j == Y)
                def _():
                    tile(mq, j, mk, True)

                @pl.when(j < Y)
                def _():
                    tile(mq, j, mk, False)

        @pl.when(mk < mq)
        def _():
            @pl.loop(0, 2)
            def _(i):
                tile2(mq, at(Y, 2 * i), at(Y, 2 * i + 1), mk)

        @pl.when((t >= 3) & (mq >= last))
        def _():
            finish(mq)

    lax.fori_loop(0, len(fourth), body, None)

    o2_forward(1)
    pass_on()
    o2_near(0)
    o2_near(1)
    o2_finish(0)
    o2_finish(1)
    got(wobuf.at[:, :, 0], o3_r)

    tn = 768

    def out_step(rels, final):
        lo = slots[rels[0]]

        @pl.loop(0, d // tn)
        def _(i):
            here = pl.ds(pl.multiple_of(i * tn, tn), tn)
            w = jnp.concatenate([wobuf[at(X, rel), :, :, :, here].reshape(width, tn) for rel in rels], axis=0)
            part = dot(seen[:, lo * width : (lo + len(rels)) * width], w)
            if final:
                yout[:, here] = (acc[:, here] + part).astype(y_ref.dtype)
                local(yout.at[:, here], y_ref.at[:, here], y_s)
            else:
                acc[:, here] = xbuf[X, :, here].astype(jnp.float32) + part

    got(seat(3), a_r.at[3])
    out_step((0, 3), False)
    got(seat(RIGHT), a_r.at[1])
    got(seat(FAR, 0, kept), a_r.at[2])
    got(seat(FAR, kept, 2 * part), a_r.at[0])
    out_step((1, 2), True)

    sent(xbuf.at[upto(3)], x_s)
    sent(wbuf.at[0, upto(3), :, upto(2 * HEAD)], w1_s)
    sent(wbuf.at[upto(3), :, :, upto(2 * HEAD)], w2_s)
    sent(wbuf.at[upto(2)], w3_s)
    sent(wobuf.at[0, upto(3), 0], o1_s)
    sent(wobuf.at[upto(3), :, 0], o2_s)
    sent(wobuf.at[:, :, 0], o3_s)
    sent(xbuf.at[:, :, upto(6 * HEAD)], kv_s)
    sent(sout.at[:, upto((3 * own + 2 * part) // n)], a_s)
    pltpu.make_async_copy(yout, y_ref, y_s).wait()


def tables(own, chunks):
    half = HEAD // 2
    rate = np.float64(THETA) ** (-np.arange(half, dtype=np.float64) / half)
    row = np.arange(own, dtype=np.float64)[:, None] * rate
    chunk = (np.arange(chunks, dtype=np.float64) * own)[:, None] * rate
    return np.concatenate([f(t) for t in (row, chunk) for f in (np.cos, np.sin)]).astype(np.float32)


def solution(mesh):
    n = math.isqrt(mesh.shape["sp"])

    def step(x, gain, wq, wk, wv, wo):
        own, d = x.shape
        g = wq.shape[1] // wk.shape[1]
        rows, orow = wq.shape[0], wo.shape[0] // 2
        angles = tables(own, n * n)
        hbm = pl.BlockSpec(memory_space=pl.ANY)
        bf, dma = jnp.bfloat16, pltpu.SemaphoreType.DMA
        return pl.pallas_call(
            functools.partial(kernel, n, g),
            out_shape=jax.ShapeDtypeStruct(x.shape, bf),
            in_specs=[hbm] * 7,
            out_specs=hbm,
            scratch_shapes=[
                pltpu.VMEM(gain.shape, bf),
                pltpu.VMEM(angles.shape, jnp.float32),
                pltpu.VMEM((n, own, d), bf),
                pltpu.VMEM((2, own // 2, d), bf),
                pltpu.VMEM((n, n, rows, 2 * g * HEAD), bf),
                pltpu.VMEM((n, n, 2, orow, d), bf),
                pltpu.VMEM((n, g * own, HEAD), bf),
                pltpu.VMEM((n, n, own, HEAD), bf),
                pltpu.VMEM((n, n, HEAD, own), bf),
                pltpu.VMEM((n, HEAD + 8, g * own), jnp.float32),
                pltpu.VMEM((n, 1, g * own), jnp.float32),
                pltpu.VMEM((n, own, g * HEAD), bf),
                pltpu.VMEM((own, n * g * HEAD), bf),
                pltpu.VMEM((2, own // 8 * 3 // 2, g * HEAD), bf),
                pltpu.VMEM((own, d), jnp.float32),
                pltpu.VMEM((own, d), bf),
                dma((2,)),
                dma(()), dma((len(PIECES),)),
                dma(()), dma((2,)), dma((2,)),
                dma(()), dma((2, 4)), dma(()), dma((2,)),
                dma(()), dma((2, 4)), dma((2,)),
                dma(()), dma((2, 6)), dma(()), dma(()),
                dma(()), dma((len(PIECES), 2)), dma((3,)), dma((3,)),
                dma(()), dma((n,)), dma((2,)),
                dma(()),
            ],
            compiler_params=pltpu.CompilerParams(collective_id=0, has_side_effects=True, vmem_limit_bytes=66_000_000),
        )(x, gain, wq, wk, wv, wo, angles)

    tokens, whole = P(("dp", "sp"), None), P("sp", None)
    return jax.shard_map(
        step,
        mesh=mesh,
        in_specs=(tokens, P(None), whole, whole, whole, whole),
        out_specs=tokens,
        check_vma=False,
    )
```

```python
import functools
import math

import jax
import jax.numpy as jnp
import numpy as np
from jax import lax
from jax.experimental import pallas as pl
from jax.experimental.pallas import tpu as pltpu
from jax.sharding import PartitionSpec as P

HEAD = 256
THETA = 10000
NEG = -1e30
HIDDEN = 2 * NEG
LOG2E = 1.4426950408889634
MESH = pl.DeviceIdType.MESH
LEFT, OWN, RIGHT, FAR = -1, 0, 1, 2

PIECES = (*((by, 2 * h, 2) for by, h in ((OWN, OWN), (OWN, RIGHT), (LEFT, OWN), (RIGHT, RIGHT), (LEFT, RIGHT), (RIGHT, OWN))), *((FAR, lo, 1) for lo in (0, 2, 1, 3)))


def upto(size):
    return pl.ds(0, size)


def pick(t, values):
    out = jnp.int32(values[-1])
    for i in range(len(values) - 2, -1, -1):
        out = jnp.where(t == i, jnp.int32(values[i]), out)
    return out


def look(t, values):
    words = [sum(v << 2 * i for i, v in enumerate(values[at : at + 15])) for at in range(0, len(values), 15)]
    word = jnp.int32(words[-1])
    for i in range(len(words) - 2, -1, -1):
        word = jnp.where(t < 15 * (i + 1), jnp.int32(words[i]), word)
    return jnp.bitwise_and(lax.shift_right_logical(word, 2 * lax.rem(t, 15)), 3)


def dot(a, b, cb=0):
    return lax.dot_general(a, b, (((1,), (cb,)), ((), ())), preferred_element_type=jnp.float32)


def kernel(n, g, x_ref, gain_hbm, wq_ref, wk_ref, wv_ref, wo_ref, angles_hbm, y_ref,
           gain_ref, angles, xbuf, xn, wbuf, wobuf, qbuf, kbuf, vbuf, mix, top, sout, seen, relay, acc, yout,
           c_l, x_s, x_r, w1_s, w1_r, w_l, w2_s, w2_r, w3_s, w3_r, o1_s, o1_r, o_l, o2_s, o2_r, o3_s, o3_r, kv_s, kv_pass, kv_near_r, kv_far_r,
           a_s, a_r, r_r, y_s):
    own, d = x_ref.shape
    half, quarter = own // 2, own // 4
    rows = wq_ref.shape[0]
    orow = wo_ref.shape[0] // 2
    width = g * HEAD
    sp, dp = lax.axis_index("sp"), lax.axis_index("dp")
    X, Y = lax.div(sp, n), lax.rem(sp, n)
    c = lax.rem(dp, 2)
    partner = {"dp": dp + 1 - 2 * c}

    def at(v, by):
        return lax.rem(v + n + by, n)

    def on_x(by):
        return {"sp": at(X, by) * n + Y}

    def on_y(by):
        return {"sp": X * n + at(Y, by)}

    def send(src, dst, ss, rs, dev):
        pltpu.make_async_remote_copy(src_ref=src, dst_ref=dst, send_sem=ss, recv_sem=rs, device_id=dev, device_id_type=MESH).start()

    def got(dst, rs):
        pltpu.make_async_remote_copy(src_ref=dst, dst_ref=dst, send_sem=rs, recv_sem=rs, device_id=partner, device_id_type=MESH).wait_recv()

    def sent(src, ss):
        pltpu.make_async_remote_copy(src_ref=src, dst_ref=src, send_sem=ss, recv_sem=ss, device_id=partner, device_id_type=MESH).wait_send()

    def local(src, dst, sem):
        pltpu.make_async_copy(src, dst, sem).start()

    local(gain_hbm, gain_ref, c_l.at[0])
    local(angles_hbm, angles, c_l.at[1])
    barrier = pltpu.get_barrier_semaphore()
    peers = [on_x(by) for by in range(1, n)] + [on_y(by) for by in range(1, n)] + [partner]
    for peer in peers:
        pl.semaphore_signal(barrier, inc=1, device_id=peer, device_id_type=MESH)
    pl.semaphore_wait(barrier, len(peers))

    def block(f, core):
        return pl.ds(pl.multiple_of((2 * f + core) * HEAD, HEAD), HEAD)

    def w_dst(f, xi):
        return wbuf.at[xi, Y, :, block(f, c)]

    def w_begin(f, src):
        for by in (1, n - 1, 2):
            send(src(at(X, by)), w_dst(f, X), w1_s, w1_r.at[f], on_x(by))
        local(src(X), w_dst(f, X), w_l.at[f])

    def head_of(ref):
        return lambda h: ref.at[:, pl.ds(pl.multiple_of(h * HEAD, HEAD), HEAD)]

    @pl.when(c == 0)
    def _():
        w_begin(0, head_of(wk_ref))

    @pl.when(c == 1)
    def _():
        w_begin(0, head_of(wv_ref))

    w_begin(1, lambda h: wq_ref.at[:, pl.ds(pl.multiple_of(h * width + c * HEAD, HEAD), HEAD)])

    def x_rows(by, lo, size):
        return xbuf.at[at(X, by), pl.ds(lo * quarter, size * quarter), :]

    for p in range(2):
        _, lo, size = PIECES[p]
        local(x_ref.at[pl.ds(lo * quarter, size * quarter), :], x_rows(0, lo, size), x_r.at[p])
    for p in (2, 3, 4, 5):
        by, lo, size = PIECES[p]
        send(x_ref.at[pl.ds(lo * quarter, size * quarter), :], x_rows(0, lo, size), x_s, x_r.at[p], on_x(-by))

    def x_forward(p):
        by = PIECES[p][0]
        for k in (0, 2):
            _, lo, size = PIECES[p + 4 + k]
            send(x_rows(by, lo, size), x_rows(by, lo, size), x_s, x_r.at[p + 4 + k], on_x(-by))

    cut = d // (3 * 128) * 128

    def o_cols(o):
        return upto(cut) if o == 0 else pl.ds(cut, d - cut)

    def o_first(o, by):
        return on_y(by) if o == 0 else on_x(by)

    def o_second(o, by):
        return on_x(by) if o == 0 else on_y(by)

    def o_block(o, by, lo=0, size=orow):
        xi, yi = (X, at(Y, by)) if o == 0 else (at(X, by), Y)
        return wobuf.at[xi, yi, c, pl.ds(lo, size), o_cols(o)]

    def o_line(o, by, lo=0, size=n):
        if o == 0:
            return wobuf.at[at(X, by), pl.ds(lo, size), c, :, o_cols(o)]
        return wobuf.at[pl.ds(lo, size), at(Y, by), c, :, o_cols(o)]

    hr, hn = orow // 2, n // 2

    def o1_begin(o):
        src = wo_ref.at[pl.ds(pl.multiple_of(c * orow, orow), orow), o_cols(o)]
        send(src, o_block(o, OWN), o1_s, o1_r.at[o, 0], o_first(o, RIGHT))
        send(src, o_block(o, OWN), o1_s, o1_r.at[o, 1], o_first(o, LEFT))
        local(src, o_block(o, OWN), o_l.at[o])

    def o1_forward(o):
        got(o_block(o, LEFT), o1_r.at[o, 0])
        send(o_block(o, LEFT, 0, hr), o_block(o, LEFT, 0, hr), o1_s, o1_r.at[o, 2], o_first(o, RIGHT))
        got(o_block(o, RIGHT), o1_r.at[o, 1])
        send(o_block(o, RIGHT, hr, hr), o_block(o, RIGHT, hr, hr), o1_s, o1_r.at[o, 3], o_first(o, LEFT))

    def o3(o, by):
        send(o_line(o, by), o_line(o, by), o3_s, o3_r, partner)

    def o2_begin(o):
        got(o_block(o, FAR, 0, hr), o1_r.at[o, 2])
        got(o_block(o, FAR, hr, hr), o1_r.at[o, 3])
        pltpu.make_async_copy(o_block(o, OWN), o_block(o, OWN), o_l.at[o]).wait()
        for k, lo in ((0, 0), (1, hn)):
            send(o_line(o, OWN, lo, hn), o_line(o, OWN, lo, hn), o2_s, o2_r.at[o, k], o_second(o, RIGHT))
        for k, lo in ((2, hn), (3, 0)):
            send(o_line(o, OWN, lo, hn), o_line(o, OWN, lo, hn), o2_s, o2_r.at[o, k], o_second(o, LEFT))
        o3(o, OWN)

    def o2_forward(o):
        got(o_line(o, LEFT, 0, hn), o2_r.at[o, 0])
        send(o_line(o, LEFT, 0, hn), o_line(o, LEFT, 0, hn), o2_s, o2_r.at[o, 4], o_second(o, RIGHT))
        got(o_line(o, RIGHT, hn, hn), o2_r.at[o, 2])
        send(o_line(o, RIGHT, hn, hn), o_line(o, RIGHT, hn, hn), o2_s, o2_r.at[o, 5], o_second(o, LEFT))

    def o2_near(o):
        got(o_line(o, LEFT, hn, hn), o2_r.at[o, 1])
        o3(o, LEFT)
        got(o_line(o, RIGHT, 0, hn), o2_r.at[o, 3])
        o3(o, RIGHT)

    def o2_finish(o):
        got(o_line(o, FAR, 0, hn), o2_r.at[o, 4])
        got(o_line(o, FAR, hn, hn), o2_r.at[o, 5])
        o3(o, FAR)

    o1_begin(0)

    step = 32

    def piece_of(p):
        lo = pl.multiple_of(pick(p, [lo for _, lo, _ in PIECES]) * quarter, quarter)
        return at(X, pick(p, [by for by, _, _ in PIECES])), lo

    def norm(p, size):
        m, lo = piece_of(p)
        slot = lax.rem(p, 2)

        @pl.loop(0, size * quarter // step)
        def _(i):
            here = pl.ds(pl.multiple_of(i * step, step), step)
            t = xbuf[m, pl.ds(pl.multiple_of(lo + i * step, step), step), :].astype(jnp.float32)
            scale = lax.rsqrt(jnp.mean(t * t, -1, keepdims=True) + 1e-6)
            xn[slot, here, :] = (t * scale * gain_ref[...].astype(jnp.float32)[None, :]).astype(jnp.bfloat16)

    def columns(p, size, i):
        w = wbuf[:, :, :, i * HEAD : (i + 1) * HEAD].reshape(n * n * rows, HEAD)
        return dot(xn[lax.rem(p, 2), : size * quarter, :], w).astype(jnp.bfloat16)

    def turned(t, m, lo):
        place = m * n + Y
        cr, sr = (angles[pl.ds(f * own + lo, t.shape[0]), :] for f in range(2))
        cc, sc = (angles[pl.ds(2 * own + f * n * n + place, 1), :] for f in range(2))
        cos, sin = cc * cr - sc * sr, sc * cr + cc * sr
        a, b = t[:, : HEAD // 2].astype(jnp.float32), t[:, HEAD // 2 :].astype(jnp.float32)
        return jnp.concatenate([a * cos - b * sin, b * cos + a * sin], -1).astype(jnp.bfloat16)

    def keys_values(p, size):
        m, lo = piece_of(p)
        kbuf[Y, m, pl.ds(lo, size * quarter), :] = turned(columns(p, size, 0), m, lo)
        vbuf[Y, m, :, pl.ds(lo, size * quarter)] = columns(p, size, 1).T

    def queries(p, size):
        m, lo = piece_of(p)
        for h in range(g):
            qbuf[m, pl.ds(pl.multiple_of(h * own + lo, quarter), size * quarter), :] = turned(columns(p, size, 2 + h), m, lo)

    def k_part(p, size, by):
        m, lo = piece_of(p)
        return kbuf.at[at(Y, by), m, pl.ds(lo, size * quarter), :]

    def v_part(p, size, by):
        m, lo = piece_of(p)
        return vbuf.at[at(Y, by), m, :, pl.ds(lo, size * quarter)]

    def group(p):
        return jnp.where(p < 2, 0, jnp.where(p < 6, 1, 2))

    def kv_send(p, size):
        k, v = k_part(p, size, 0), v_part(p, size, 0)
        send(k, k, kv_s, kv_pass.at[p, 0], on_y(RIGHT))
        send(v, v, kv_s, kv_pass.at[p, 1], on_y(LEFT))
        send(k, k, kv_s, kv_near_r.at[group(p)], on_y(LEFT))
        send(v, v, kv_s, kv_near_r.at[group(p)], on_y(RIGHT))

    def kv_forward(*ps):
        for p in ps:
            k, v = k_part(p, PIECES[p][2], -1), v_part(p, PIECES[p][2], 1)
            got(k, kv_pass.at[p, 0])
            send(k, k, kv_s, kv_far_r.at[group(p)], on_y(RIGHT))
            got(v, kv_pass.at[p, 1])
            send(v, v, kv_s, kv_far_r.at[group(p)], on_y(LEFT))

    def kv_got(i, sem):
        got(kbuf.at[0, upto((2, 4, 2)[i])], sem.at[i])

    e = HEAD**-0.5 * LOG2E

    def heads(h):
        return slice(h * own, (h + 1) * own)

    def tile(mq, j, mk, masked):
        keys = kbuf[j, mk]
        scores = [dot(keys, qbuf[mq, heads(h), :], 1) for h in range(g)]
        weights, keeps = [], []
        for h, s in enumerate(scores):
            at_h = heads(h)
            if masked:
                ok = lax.broadcasted_iota(jnp.int32, s.shape, 0) <= lax.broadcasted_iota(jnp.int32, s.shape, 1)
                s = jnp.where(ok, s, HIDDEN)
            old = top[mq, :, at_h]
            new = jnp.maximum(old, s.max(axis=0, keepdims=True))
            top[mq, :, at_h] = new
            weights.append(jnp.exp2((s - new) * e).astype(jnp.bfloat16))
            keeps.append(jnp.exp2((old - new) * e))
        values = jnp.concatenate([vbuf[j, mk], jnp.ones((8, own), jnp.bfloat16)], axis=0)
        for h in range(g):
            at_h = heads(h)
            mix[mq, :, at_h] = mix[mq, :, at_h] * keeps[h] + dot(values, weights[h])

    def tile2(mq, j0, j1, mk):
        js = (j0, j1)
        scores = [[dot(kbuf[j, mk], qbuf[mq, heads(h), :], 1) for j in js] for h in range(g)]
        weights, keeps = [], []
        for h, pair_ in enumerate(scores):
            at_h = heads(h)
            old = top[mq, :, at_h]
            new = functools.reduce(jnp.maximum, [s.max(axis=0, keepdims=True) for s in pair_], old)
            top[mq, :, at_h] = new
            weights.append(jnp.concatenate([jnp.exp2((s - new) * e).astype(jnp.bfloat16) for s in pair_], axis=0))
            keeps.append(jnp.exp2((old - new) * e))
        values = jnp.concatenate([jnp.concatenate([vbuf[j, mk] for j in js], axis=1), jnp.ones((8, 2 * own), jnp.bfloat16)], axis=0)
        for h in range(g):
            at_h = heads(h)
            mix[mq, :, at_h] = mix[mq, :, at_h] * keeps[h] + dot(values, weights[h])

    def later(ra, rb):
        ma, mb = at(X, ra), at(X, rb)
        return jnp.maximum(ma, mb), jnp.minimum(ma, mb)

    def singles(table, before=None):
        def body(t, _):
            for i, todo in (before or {}).items():

                @pl.when(t == i)
                def _(todo=todo):
                    todo()

            ra, rb, by = (look(t, [row[k] % n for row in table]) for k in range(3))
            (mq, mk), j = later(ra, rb), at(Y, by)
            q_place, k_place = mq * n + Y, mk * n + j

            @pl.when(k_place == q_place)
            def _():
                tile(mq, j, mk, True)

            @pl.when(k_place < q_place)
            def _():
                tile(mq, j, mk, False)

        lax.fori_loop(0, len(table), body, None)

    def cross(pairs, *places):
        return [(a, b, by) for by in places for a, b in pairs]

    last = at(X, FAR)
    slots = (0, 2, 3, 1)

    def seat(rel, lo=0, size=own):
        return seen.at[pl.ds(lo, size), pl.ds(pl.multiple_of(pick(rel, slots) * width, width), width)]

    part = own // 8
    kept = own - 2 * part

    def finish(mq):
        out = mix[mq, :HEAD, :] * (1 / mix[mq, HEAD : HEAD + 1, :])
        to = at(mq, -X)
        back = at(X, -mq)
        for h in range(g):
            sout[mq, :, h * HEAD : (h + 1) * HEAD] = out[:, heads(h)].T.astype(jnp.bfloat16)

        @pl.when(to == 0)
        def _():
            seen[:, :width] = sout[mq]

        @pl.when(to == 2)
        def _():
            for i in range(2):
                send(sout.at[mq, pl.ds(kept + i * part, part), :], relay.at[i], a_s, r_r.at[i], on_x(LEFT))
            send(sout.at[mq, upto(kept), :], seat(FAR, 0, kept), a_s, a_r.at[2], on_x(FAR))

        @pl.when((to == 1) | (to == 3))
        def _():
            send(sout.at[mq], seat(back), a_s, a_r.at[back], {"sp": mq * n + Y})

    def pass_on():
        for i in range(2):
            got(relay.at[i], r_r.at[i])
            send(relay.at[i], seat(FAR, kept + i * part, part), a_s, a_r.at[0], on_x(LEFT))

    top[...] = jnp.full(top.shape, NEG, jnp.float32)

    @pl.loop(0, n)
    def _(m):
        mix[m] = jnp.zeros(mix.shape[1:], jnp.float32)

    def arrive(p, size):
        got(xbuf.at[0, upto(size * quarter), :], x_r.at[p])

    def pair(a, size, f):
        lax.fori_loop(a, a + 2, lambda p, _: f(p, size), None)

    def early_half(p, size):
        norm(p, size)
        keys_values(p, size)
        kv_send(p, size)

    pltpu.make_async_copy(gain_hbm, gain_ref, c_l.at[0]).wait()
    pltpu.make_async_copy(angles_hbm, angles, c_l.at[1]).wait()
    arrive(0, 2)
    arrive(1, 2)
    pair(0, 2, norm)

    def w_line(f, by, lo=0, size=n):
        return wbuf.at[pl.ds(lo, size), at(Y, by), :, block(f, c)]

    def w3(f, by):
        send(w_line(f, by), w_line(f, by), w3_s, w3_r.at[f], partner)

    def w2_begin(f):
        got(wbuf.at[0, upto(n - 1), :, upto(HEAD)], w1_r.at[f])
        pltpu.make_async_copy(w_dst(f, X), w_dst(f, X), w_l.at[f]).wait()
        send(w_line(f, OWN), w_line(f, OWN), w2_s, w2_r.at[f, 0], on_y(RIGHT))
        send(w_line(f, OWN), w_line(f, OWN), w2_s, w2_r.at[f, 1], on_y(LEFT))
        w3(f, OWN)

    def w2_forward(f):
        got(w_line(f, LEFT), w2_r.at[f, 0])
        send(w_line(f, LEFT, 0, hn), w_line(f, LEFT, 0, hn), w2_s, w2_r.at[f, 2], on_y(RIGHT))
        got(w_line(f, RIGHT), w2_r.at[f, 1])
        send(w_line(f, RIGHT, hn, hn), w_line(f, RIGHT, hn, hn), w2_s, w2_r.at[f, 3], on_y(LEFT))
        w3(f, LEFT)
        w3(f, RIGHT)

    def w2_finish(f):
        got(w_line(f, FAR, 0, hn), w2_r.at[f, 2])
        got(w_line(f, FAR, hn, hn), w2_r.at[f, 3])
        w3(f, FAR)

    def w3_wait(f):
        got(wbuf.at[:, :, :, upto(HEAD)], w3_r.at[f])

    w2_begin(0)
    o1_forward(0)
    w2_forward(0)
    w2_begin(1)
    w2_finish(0)
    w3_wait(0)
    pair(0, 2, keys_values)
    w2_forward(1)
    pair(0, 2, kv_send)
    w2_finish(1)
    w3_wait(1)
    pair(0, 2, queries)

    for p in (2, 3):
        arrive(p, 2)
        x_forward(p)
    pair(2, 2, early_half)
    kv_forward(0, 1)
    pair(2, 2, queries)
    o1_begin(1)
    singles(cross([(OWN, OWN)], OWN, RIGHT, LEFT), {1: lambda: kv_got(0, kv_near_r)})
    kv_forward(2, 3)

    arrive(4, 2)
    arrive(5, 2)
    pair(4, 2, early_half)
    pair(4, 2, queries)
    pairs, same = [(OWN, LEFT), (OWN, RIGHT), (LEFT, RIGHT)], [(LEFT, LEFT), (RIGHT, RIGHT)]
    singles(cross([(OWN, OWN)], FAR) + cross(pairs + same, OWN), {0: lambda: kv_got(0, kv_far_r)})

    arrive(6, 1)
    arrive(7, 1)
    pair(6, 1, early_half)
    pair(6, 1, queries)
    kv_forward(4, 5)
    kv_got(1, kv_near_r)

    @pl.loop(0, len(pairs))
    def _(t):
        mq, mk = later(look(t, [a % n for a, _ in pairs]), look(t, [b % n for _, b in pairs]))
        tile2(mq, at(Y, RIGHT), at(Y, LEFT), mk)

    singles(cross(same, RIGHT, LEFT))
    kv_forward(6, 7)

    arrive(8, 1)
    arrive(9, 1)
    pair(8, 1, early_half)
    pair(8, 1, queries)

    o1_forward(1)
    o2_begin(0)
    kv_got(1, kv_far_r)
    singles(cross(pairs + same, FAR))

    kv_forward(8, 9)
    o2_begin(1)

    @pl.loop(0, n)
    def _(mq):
        @pl.when(mq < last)
        def _():
            finish(mq)


    fourth = [*((FAR, by) for by in (OWN, LEFT, RIGHT, FAR)), *((by, FAR) for by in (RIGHT, LEFT, OWN))]

    def body(t, _):
        rq, rk = (look(t, [row[k] % n for row in fourth]) for k in range(2))
        mq, mk = at(X, rq), at(X, rk)

        @pl.when(t == 3)
        def _():
            o2_forward(0)
            kv_got(2, kv_near_r)
            kv_got(2, kv_far_r)

            @pl.loop(0, n)
            def _(j):
                @pl.when(j == Y)
                def _():
                    tile(mq, j, mk, True)

                @pl.when(j < Y)
                def _():
                    tile(mq, j, mk, False)

        @pl.when(mk < mq)
        def _():
            @pl.loop(0, 2)
            def _(i):
                tile2(mq, at(Y, 2 * i), at(Y, 2 * i + 1), mk)

        @pl.when((t >= 3) & (mq >= last))
        def _():
            finish(mq)

    lax.fori_loop(0, len(fourth), body, None)

    o2_forward(1)
    pass_on()
    o2_near(0)
    o2_near(1)
    o2_finish(0)
    o2_finish(1)
    got(wobuf.at[:, :, 0], o3_r)

    tn = 768

    def out_step(rels, final):
        lo = slots[rels[0]]

        @pl.loop(0, d // tn)
        def _(i):
            here = pl.ds(pl.multiple_of(i * tn, tn), tn)
            w = jnp.concatenate([wobuf[at(X, rel), :, :, :, here].reshape(width, tn) for rel in rels], axis=0)
            part = dot(seen[:, lo * width : (lo + len(rels)) * width], w)
            if final:
                yout[:, here] = (acc[:, here] + part).astype(y_ref.dtype)
                local(yout.at[:, here], y_ref.at[:, here], y_s)
            else:
                acc[:, here] = xbuf[X, :, here].astype(jnp.float32) + part

    got(seat(3), a_r.at[3])
    out_step((0, 3), False)
    got(seat(RIGHT), a_r.at[1])
    got(seat(FAR, 0, kept), a_r.at[2])
    got(seat(FAR, kept, 2 * part), a_r.at[0])
    out_step((1, 2), True)

    sent(xbuf.at[upto(3)], x_s)
    sent(wbuf.at[0, upto(3), :, upto(2 * HEAD)], w1_s)
    sent(wbuf.at[upto(3), :, :, upto(2 * HEAD)], w2_s)
    sent(wbuf.at[upto(2)], w3_s)
    sent(wobuf.at[0, upto(3), 0], o1_s)
    sent(wobuf.at[upto(3), :, 0], o2_s)
    sent(wobuf.at[:, :, 0], o3_s)
    sent(xbuf.at[:, :, upto(6 * HEAD)], kv_s)
    sent(sout.at[:, upto((3 * own + 2 * part) // n)], a_s)
    pltpu.make_async_copy(yout, y_ref, y_s).wait()


def tables(own, chunks):
    half = HEAD // 2
    rate = np.float64(THETA) ** (-np.arange(half, dtype=np.float64) / half)
    row = np.arange(own, dtype=np.float64)[:, None] * rate
    chunk = (np.arange(chunks, dtype=np.float64) * own)[:, None] * rate
    return np.concatenate([f(t) for t in (row, chunk) for f in (np.cos, np.sin)]).astype(np.float32)


def solution(mesh):
    n = math.isqrt(mesh.shape["sp"])

    def step(x, gain, wq, wk, wv, wo):
        own, d = x.shape
        g = wq.shape[1] // wk.shape[1]
        rows, orow = wq.shape[0], wo.shape[0] // 2
        angles = tables(own, n * n)
        hbm = pl.BlockSpec(memory_space=pl.ANY)
        bf, dma = jnp.bfloat16, pltpu.SemaphoreType.DMA
        return pl.pallas_call(
            functools.partial(kernel, n, g),
            out_shape=jax.ShapeDtypeStruct(x.shape, bf),
            in_specs=[hbm] * 7,
            out_specs=hbm,
            scratch_shapes=[
                pltpu.VMEM(gain.shape, bf),
                pltpu.VMEM(angles.shape, jnp.float32),
                pltpu.VMEM((n, own, d), bf),
                pltpu.VMEM((2, own // 2, d), bf),
                pltpu.VMEM((n, n, rows, 2 * g * HEAD), bf),
                pltpu.VMEM((n, n, 2, orow, d), bf),
                pltpu.VMEM((n, g * own, HEAD), bf),
                pltpu.VMEM((n, n, own, HEAD), bf),
                pltpu.VMEM((n, n, HEAD, own), bf),
                pltpu.VMEM((n, HEAD + 8, g * own), jnp.float32),
                pltpu.VMEM((n, 1, g * own), jnp.float32),
                pltpu.VMEM((n, own, g * HEAD), bf),
                pltpu.VMEM((own, n * g * HEAD), bf),
                pltpu.VMEM((2, own // 8, g * HEAD), bf),
                pltpu.VMEM((own, d), jnp.float32),
                pltpu.VMEM((own, d), bf),
                dma((2,)),
                dma(()), dma((len(PIECES),)),
                dma(()), dma((2,)), dma((2,)),
                dma(()), dma((2, 4)), dma(()), dma((2,)),
                dma(()), dma((2, 4)), dma((2,)),
                dma(()), dma((2, 6)), dma(()), dma(()),
                dma(()), dma((len(PIECES), 2)), dma((3,)), dma((3,)),
                dma(()), dma((n,)), dma((2,)),
                dma(()),
            ],
            compiler_params=pltpu.CompilerParams(collective_id=0, has_side_effects=True, vmem_limit_bytes=66_000_000),
        )(x, gain, wq, wk, wv, wo, angles)

    tokens, whole = P(("dp", "sp"), None), P("sp", None)
    return jax.shard_map(
        step,
        mesh=mesh,
        in_specs=(tokens, P(None), whole, whole, whole, whole),
        out_specs=tokens,
        check_vma=False,
    )
```
